32 devices in a mesh: kx: 8 (over z, x), cz: 4 (over y, core).
Axes of the slice: x: 2, y: 2, z: 4, core: 2. Of those that a mesh axis runs over, the one named last changes fastest.
Arguments:
- field_modes: bfloat16 [512, 4, 12288], P('cz', None, 'kx'), may hold values from -6 to 6
- cotangent: bfloat16 [512, 4, 12288], P('cz', None, 'kx'), may hold values from -6 to 6
Outputs:
- mode_gradient: bfloat16 [512, 4, 12288], P('cz', None, 'kx')
The draws below stay inside these ranges and needn't reach their ends.
All inputs are finite; a program needn't handle non-finite values.
Results may differ from the reference program's by a relative error of at most 0.009.
Values may be sent and summed in bfloat16 or wider, within the bound.
A program may use at most 128 MiB of HBM per device.

```python
import math
import jax
import jax.numpy as jnp
from jax import lax

FIELDS = 4
NZ = 512
MZ = 768
NX = 768
Y = 16


def steps_of(key, dims, pieces, smallest, largest):
    gain, own = 1.0, jax.random.fold_in(key, 6)
    for axis_at, shards_of in pieces:
        heights = jnp.exp(jax.random.uniform(jax.random.fold_in(own, axis_at), (shards_of,), jnp.float32, smallest / len(pieces), largest / len(pieces)))
        gain = gain * jnp.repeat(heights, dims[axis_at] // shards_of).reshape([-1 if axis == axis_at else 1 for axis in range(len(dims))])
    return gain


def normal_values(rng, shape, spread, bound, cuts=(), kind=jnp.bfloat16):
    factor_of = steps_of(rng, shape, cuts, -0.22, 0.18) if cuts else 1.0
    drawn = jax.random.normal(rng, shape, jnp.float32) * spread * factor_of
    return jnp.minimum(jnp.maximum(drawn, -bound), bound).astype(kind)


def setup_inputs(seed: int = 0) -> dict:
    key_of = jax.random.split(jax.random.key(seed), 3)
    return {
        "field_modes": normal_values(key_of[0], (NZ, FIELDS, NX * Y), 1.0, 6.0, ((0, 4), (2, 8))),
        "cotangent": normal_values(key_of[1], (NZ, FIELDS, NX * Y), 1.0, 6.0, ((0, 4), (2, 8))),
    }


def cosine_table():
    row_index = jnp.arange(MZ, dtype=jnp.int32)
    col_index = jnp.arange(NZ, dtype=jnp.int32)
    position = col_index[None, :] * (2 * row_index[:, None] + 1) % (4 * MZ)
    return jnp.cos(jnp.pi * position.astype(jnp.float32) / (2 * MZ))

def hartley_table():
    points = jnp.arange(NX, dtype=jnp.int32)
    position = points[:, None] * points[None, :] % NX
    phases = 2.0 * jnp.pi * position.astype(jnp.float32) / NX
    return ((jnp.cos(phases) + jnp.sin(phases)) / math.sqrt(NX)).astype(jnp.bfloat16)

def product_gradient(fields, adjoint):
    vertical = fields[2]
    return jnp.stack([adjoint[0] * vertical, adjoint[1] * vertical, adjoint[0] * fields[0] + adjoint[1] * fields[1] + 2.0 * adjoint[2] * vertical + adjoint[3] * fields[3], adjoint[3] * vertical]).astype(jnp.bfloat16)

def reference(field_modes, cotangent):
    highest = lax.Precision.HIGHEST
    field_grid = field_modes.reshape(NZ, FIELDS, NX, Y)
    cotangent_grid = cotangent.reshape(NZ, FIELDS, NX, Y)
    cosines = cosine_table()
    synthesis_full = (cosines * math.sqrt(2.0 / NZ)).astype(jnp.bfloat16).astype(jnp.float32)
    projection_full = (cosines * math.sqrt(2.0 / MZ)).astype(jnp.bfloat16).astype(jnp.float32)
    hartley_full = hartley_table().astype(jnp.float32)
    block_rows = 8
    block_count = Y // block_rows

    def one_block(position):
        first_row = position * block_rows
        mode_block = lax.dynamic_slice_in_dim(field_grid, first_row, block_rows, 3).astype(jnp.float32)
        adjoint_block = lax.dynamic_slice_in_dim(cotangent_grid, first_row, block_rows, 3).astype(jnp.float32)
        lifted_fields = jnp.einsum('zk,kfmy->fzmy', synthesis_full, mode_block, precision=highest).astype(jnp.bfloat16).astype(jnp.float32)
        lifted_adjoint = jnp.einsum('zk,kfmy->fzmy', projection_full, adjoint_block, precision=highest).astype(jnp.bfloat16).astype(jnp.float32)
        fields = jnp.einsum('xm,fzmy->fzxy', hartley_full, lifted_fields, precision=highest)
        adjoint = jnp.einsum('xm,fzmy->fzxy', hartley_full, lifted_adjoint, precision=highest)
        gradient = product_gradient(fields, adjoint).astype(jnp.float32)
        turned = jnp.einsum('xm,fzxy->fzmy', hartley_full, gradient, precision=highest).astype(jnp.bfloat16).astype(jnp.float32)
        spectral = jnp.einsum('zk,fzmy->kfmy', synthesis_full, turned, precision=highest)
        return spectral.astype(jnp.bfloat16)
    blocks = lax.map(one_block, jnp.arange(block_count, dtype=jnp.int32))
    return jnp.moveaxis(blocks, 0, 3).reshape(NZ, FIELDS, NX * Y)
```

```python
import functools
import math

import jax
import jax.numpy as jnp
import numpy as np
from jax import lax
from jax.experimental import pallas as pl
from jax.experimental.pallas import tpu as pltpu
from jax.sharding import PartitionSpec as P

MZ = 768
Y = 16
MESH = pl.DeviceIdType.MESH


def cosine_table(rows, columns):
    position = (np.arange(columns)[None, :] * (2 * np.arange(rows)[:, None] + 1)) % (4 * rows)
    return np.cos(np.pi * position / (2 * rows)).astype(np.float32)


def hartley_table(points):
    index = np.arange(points)
    phases = 2.0 * np.pi * ((index[:, None] * index[None, :]) % points) / points
    return (np.cos(phases) + np.sin(phases)) / math.sqrt(points)


def matmul(a, b):
    return jnp.dot(a, b, preferred_element_type=jnp.float32)


def matmul_t(a, b):
    return lax.dot_general(a, b, (((1,), (1,)), ((), ())), preferred_element_type=jnp.float32)


def kernel(
    nkx, ncz, pieces,
    field_modes, cotangent, tables_in,
    out,
    raw, tables, raw_sem, table_sem, ready,
    wide, rows, held, mixed, parts, points, total, flux, lowered, turned, result, landed,
    in_send, in_recv, swap_send, swap_recv, back_send, back_recv, out_send, out_recv,
):
    local_k, fields, columns = field_modes.shape
    rows_y = rows.shape[1]
    local_m = columns // rows_y
    own_rows = rows_y // nkx
    points_x = local_m * nkx
    points_z = points.shape[2]
    modes_z = local_k * ncz
    share_x = points_x // ncz
    aligned = local_k % 128 == 0
    i, j = lax.axis_index("kx"), lax.axis_index("cz")
    order = ((0, 2), (1, 0), (1, 1), (1, 3), (0, 0), (0, 1), (0, 3), (1, 2))

    places = nkx // 2
    place, column = i // 2, lax.rem(i, 2)
    above, below = place + 1 < places, place > 0
    near = 1 + jnp.where(above, 1, 0) + jnp.where(below, 1, 0)

    def at(row_owner, mode_owner):
        return {"kx": row_owner, "cz": mode_owner}

    def wait(ref, sem):
        pltpu.make_async_copy(ref, ref, sem).wait()

    piece = columns // pieces
    raw_copies = [
        [
            pltpu.make_async_copy(
                array.at[:, :, pl.ds(p * piece, piece)], raw.at[a, :, :, pl.ds(p * piece, piece)], raw_sem.at[a, p]
            )
            for p in range(pieces)
        ]
        for a, array in enumerate((field_modes, cotangent))
    ]
    table_copy = pltpu.make_async_copy(tables_in, tables, table_sem)
    for copy in raw_copies[0]:
        copy.start()
    barrier = pltpu.get_barrier_semaphore()

    def signal_near(sem):
        pl.semaphore_signal(sem, inc=1, device_id=at(place * 2 + 1 - column, j), device_id_type=MESH)

        @pl.when(above)
        def _():
            pl.semaphore_signal(sem, inc=1, device_id=at(i + 2, j), device_id_type=MESH)

        @pl.when(below)
        def _():
            pl.semaphore_signal(sem, inc=1, device_id=at(i - 2, j), device_id_type=MESH)

    signal_near(barrier)
    for step in range(1, ncz):
        pl.semaphore_signal(barrier, inc=1, device_id=at(i, lax.rem(j + step, ncz)), device_id_type=MESH)
    for copy in raw_copies[1]:
        copy.start()

    hartley = tables.at[pl.ds(0, points_x)]
    lifts = [tables.at[pl.ds(points_x + n * modes_z, modes_z)] for n in range(2)]
    chunk = 128 if piece % 128 == 0 else piece

    def prepare(h):
        a, f = order[h]

        def turn(step, carry):
            here = pl.ds(pl.multiple_of(step * chunk, chunk), chunk)
            wide[here, :] = raw[a, :, f, here].astype(jnp.float32).T
            return carry

        for p in range(pieces):
            if h < 2:
                raw_copies[a][p].wait()
                lax.fori_loop(p * (piece // chunk), (p + 1) * (piece // chunk), turn, 0)
        if h >= 2:
            lax.fori_loop(0, columns // chunk, turn, 0)
        for y in range(rows_y):
            rows[h, y] = wide[pl.ds(y, local_m, stride=rows_y), :].astype(jnp.bfloat16)

    def in_place(h):
        return held.at[h, :, pl.ds(pl.multiple_of(i * local_m, local_m), local_m)]

    def send_in(h, target):
        pltpu.make_async_remote_copy(
            src_ref=rows.at[h, pl.ds(target * own_rows, own_rows)],
            dst_ref=in_place(h),
            send_sem=in_send,
            recv_sem=in_recv.at[h],
            device_id=at(target, j),
            device_id_type=MESH,
        ).start()

    def keep_in(h):
        pltpu.make_async_copy(rows.at[h, pl.ds(i * own_rows, own_rows)], in_place(h), in_recv.at[h]).start()

    def flip(index, step):
        bit = 1
        target = index
        while bit < nkx:
            if step & bit:
                target = target + bit * (1 - 2 * lax.rem(index // bit, 2))
            bit *= 2
        return target

    half = nkx // 2
    steps = [s for s in range(1, half)] + [s for s in range(half, nkx) if s % 2] + [s for s in range(half, nkx) if not s % 2]

    def others():
        if nkx & (nkx - 1):
            return [lax.rem(i + s, nkx) for s in range(1, nkx)]
        return [flip(i, s) for s in steps]

    def send_at_distance(h, distance):
        for hops, side in ((distance, 0), (distance - 1, 1)):
            facing = place * 2 + (column if side == 0 else 1 - column)
            if hops == 0:
                send_in(h, facing)
            elif hops < places:
                @pl.when(place + hops < places)
                def _():
                    send_in(h, facing + 2 * hops)

                @pl.when(place >= hops)
                def _():
                    send_in(h, facing - 2 * hops)

    prepare(0)
    pl.semaphore_wait(barrier, near + ncz - 1)
    send_at_distance(0, 1)
    for distance in range(2, places + 1):
        sem = ready.at[distance - 2]
        signal_near(sem)
        pl.semaphore_wait(sem, near)
        send_at_distance(0, distance)
    keep_in(0)
    table_copy.start()
    for h in range(1, 2 * fields):
        prepare(h)
        for target in others():
            send_in(h, target)
        keep_in(h)

    def share_rows(q):
        return pl.ds(pl.multiple_of(q * share_x, share_x), share_x)

    def lanes(r):
        return slice(r * local_k, (r + 1) * local_k)

    def transform(target, source):
        if aligned:
            joined = source[0] if len(source) == 1 else jnp.concatenate(source, axis=1)
            value = matmul(hartley[...], joined).astype(jnp.bfloat16)
            for r in range(own_rows):
                target(r, value[:, lanes(r)])
        else:
            for r in range(own_rows):
                target(r, matmul(hartley[...], source[r]).astype(jnp.bfloat16))

    def mix(h):
        wait(held.at[h], in_recv.at[h])

        def keep(r, value):
            mixed[h, :, lanes(r)] = value

        transform(keep, [held[h, r] for r in range(own_rows)])
        for step in range(1, ncz):
            q = lax.rem(j + step, ncz)
            pltpu.make_async_remote_copy(
                src_ref=mixed.at[h, share_rows(q), :],
                dst_ref=parts.at[h, j],
                send_sem=swap_send,
                recv_sem=swap_recv.at[h],
                device_id=at(i, q),
                device_id_type=MESH,
            ).start()
        pltpu.make_async_copy(mixed.at[h, share_rows(j), :], parts.at[h, j], swap_recv.at[h]).start()

    block_z = 256 if points_z % 256 == 0 else points_z

    def lift(h, use):
        wait(parts.at[h], swap_recv.at[h])
        table = lifts[order[h][0]]

        def one(step, carry):
            here = pl.ds(pl.multiple_of(step * block_z, block_z), block_z)
            if aligned:
                joined = jnp.concatenate(
                    [
                        jnp.concatenate([parts[h, q, :, lanes(r)] for q in range(ncz)], axis=1)
                        for r in range(own_rows)
                    ],
                    axis=0,
                )
                use(slice(None), here, matmul(joined, table[:, here]))
            else:
                for r in range(own_rows):
                    value = matmul(parts[h, 0, :, lanes(r)], table[0:local_k, here])
                    for q in range(1, ncz):
                        value += matmul(parts[h, q, :, lanes(r)], table[q * local_k:(q + 1) * local_k, here])
                    use(slice(r * share_x, (r + 1) * share_x), here, value)
            return carry

        lax.fori_loop(0, points_z // block_z, one, 0)

    def leave(f):
        if aligned:
            value = matmul_t(flux[...], lifts[0][...]).astype(jnp.bfloat16)
            for q in range(ncz):
                for r in range(own_rows):
                    lowered[f, q, :, lanes(r)] = value[r * share_x:(r + 1) * share_x, lanes(q)]
        else:
            for q in range(ncz):
                for r in range(own_rows):
                    lowered[f, q, :, lanes(r)] = matmul_t(
                        flux[r * share_x:(r + 1) * share_x, :], lifts[0][q * local_k:(q + 1) * local_k, :]
                    ).astype(jnp.bfloat16)
        for step in range(1, ncz):
            q = lax.rem(j + step, ncz)
            pltpu.make_async_remote_copy(
                src_ref=lowered.at[f, q],
                dst_ref=turned.at[f, share_rows(j), :],
                send_sem=back_send,
                recv_sem=back_recv.at[f],
                device_id=at(i, q),
                device_id_type=MESH,
            ).start()
        pltpu.make_async_copy(lowered.at[f, j], turned.at[f, share_rows(j), :], back_recv.at[f]).start()

    def out_block(f, target):
        return result.at[f, :, pl.ds(pl.multiple_of(target * local_m, local_m), local_m)]

    def out_place(f):
        return landed.at[f, pl.ds(i * own_rows, own_rows)]

    def finish(f):
        wait(turned.at[f], back_recv.at[f])

        def keep(r, value):
            result[f, r] = value

        transform(keep, [turned[f, :, lanes(r)] for r in range(own_rows)])
        for target in others():
            pltpu.make_async_remote_copy(
                src_ref=out_block(f, target),
                dst_ref=out_place(f),
                send_sem=out_send,
                recv_sem=out_recv.at[f],
                device_id=at(target, j),
                device_id_type=MESH,
            ).start()
        pltpu.make_async_copy(out_block(f, i), out_place(f), out_recv.at[f]).start()

    def keep(h):
        def use(part, here, value):
            points[h, part, here] = value
        return use

    def keep_and_flux(h):
        def use(part, here, value):
            points[h, part, here] = value
            flux[part, here] = (value * points[0, part, here]).astype(jnp.bfloat16)
        return use

    def first(part, here, value):
        total[part, here] = points[1, part, here] * value

    def add(h):
        def use(part, here, value):
            total[part, here] += points[h, part, here] * value
        return use

    def last(part, here, value):
        flux[part, here] = (total[part, here] + 2.0 * value * points[0, part, here]).astype(jnp.bfloat16)

    table_copy.wait()
    mix(0)
    mix(1)
    lift(0, keep(0))
    lift(1, keep_and_flux(1))
    leave(0)
    mix(2)
    finish(0)
    lift(2, keep_and_flux(2))
    leave(1)
    mix(3)
    finish(1)
    lift(3, keep_and_flux(3))
    leave(3)
    mix(4)
    finish(3)
    lift(4, first)
    mix(5)
    lift(5, add(2))
    mix(6)
    lift(6, add(3))
    mix(7)
    lift(7, last)
    leave(2)
    finish(2)

    for f in (0, 1, 3, 2):
        wait(landed.at[f], out_recv.at[f])
        for y in range(rows_y):
            wide[pl.ds(y, local_m, stride=rows_y), :] = landed[f, y].astype(jnp.float32)

        def settle(step, carry):
            here = pl.ds(pl.multiple_of(step * chunk, chunk), chunk)
            out[f, here, :] = wide[here, :].astype(jnp.bfloat16)
            return carry

        lax.fori_loop(0, columns // chunk, settle, 0)

    wait(rows.at[:, pl.ds(0, rows_y - own_rows)], in_send)
    wait(mixed.at[:, pl.ds(0, points_x - share_x), :], swap_send)
    wait(lowered.at[:, pl.ds(0, ncz - 1)], back_send)
    wait(landed.at[:, pl.ds(0, rows_y - own_rows)], out_send)


def on_device(nkx, ncz, field_modes, cotangent):
    local_k, fields, columns = field_modes.shape
    local_m = columns // Y
    modes_z, points_x = local_k * ncz, local_m * nkx
    own_rows = Y // nkx
    share_x = points_x // ncz
    bf16 = jnp.bfloat16
    pieces = next(p for p in (4, 3, 2, 1) if columns % (p * 128) == 0 or p == 1)

    cosines = cosine_table(MZ, modes_z)
    synthesis = (cosines * math.sqrt(2.0 / modes_z)).astype(bf16).T
    projection = (cosines * math.sqrt(2.0 / MZ)).astype(bf16).T
    hartley = hartley_table(points_x).astype(np.float32).astype(bf16)
    tables = jnp.asarray(np.concatenate([hartley, synthesis, projection], axis=0))

    hbm = pl.BlockSpec(memory_space=pltpu.HBM)
    dma = pltpu.SemaphoreType.DMA
    out = pl.pallas_call(
        functools.partial(kernel, nkx, ncz, pieces),
        out_shape=jax.ShapeDtypeStruct((fields, columns, local_k), bf16),
        in_specs=[hbm] * 3,
        out_specs=pl.BlockSpec(memory_space=pltpu.VMEM),
        scratch_shapes=[
            pltpu.VMEM((2, local_k, fields, columns), bf16),
            pltpu.VMEM(tables.shape, bf16),
            dma((2, pieces)), dma, pltpu.SemaphoreType.REGULAR((nkx // 2,)),
            pltpu.VMEM((columns, local_k), jnp.float32),
            pltpu.VMEM((2 * fields, Y, local_m, local_k), bf16),
            pltpu.VMEM((2 * fields, own_rows, points_x, local_k), bf16),
            pltpu.VMEM((2 * fields, points_x, own_rows * local_k), bf16),
            pltpu.VMEM((2 * fields, ncz, share_x, own_rows * local_k), bf16),
            pltpu.VMEM((fields, own_rows * share_x, MZ), jnp.float32),
            pltpu.VMEM((own_rows * share_x, MZ), jnp.float32),
            pltpu.VMEM((own_rows * share_x, MZ), bf16),
            pltpu.VMEM((fields, ncz, share_x, own_rows * local_k), bf16),
            pltpu.VMEM((fields, points_x, own_rows * local_k), bf16),
            pltpu.VMEM((fields, own_rows, points_x, local_k), bf16),
            pltpu.VMEM((fields, Y, local_m, local_k), bf16),
            dma, dma((2 * fields,)), dma, dma((2 * fields,)),
            dma, dma((fields,)), dma, dma((fields,)),
        ],
        compiler_params=pltpu.CompilerParams(has_side_effects=True, vmem_limit_bytes=52 * 2**20, collective_id=0),
    )(field_modes, cotangent, tables)
    return out.transpose(2, 0, 1)


def solution(mesh):
    return jax.shard_map(
        functools.partial(on_device, mesh.shape["kx"], mesh.shape["cz"]),
        mesh=mesh,
        in_specs=(P("cz", None, "kx"), P("cz", None, "kx")),
        out_specs=P("cz", None, "kx"),
        check_vma=False,
    )
```

```python
import functools
import math

import jax
import jax.numpy as jnp
import numpy as np
from jax import lax
from jax.experimental import pallas as pl
from jax.experimental.pallas import tpu as pltpu
from jax.sharding import PartitionSpec as P

MZ = 768
Y = 16
MESH = pl.DeviceIdType.MESH


def cosine_table(rows, columns):
    position = (np.arange(columns)[None, :] * (2 * np.arange(rows)[:, None] + 1)) % (4 * rows)
    return np.cos(np.pi * position / (2 * rows)).astype(np.float32)


def hartley_table(points):
    index = np.arange(points)
    phases = 2.0 * np.pi * ((index[:, None] * index[None, :]) % points) / points
    return (np.cos(phases) + np.sin(phases)) / math.sqrt(points)


def matmul(a, b):
    return jnp.dot(a, b, preferred_element_type=jnp.float32)


def matmul_t(a, b):
    return lax.dot_general(a, b, (((1,), (1,)), ((), ())), preferred_element_type=jnp.float32)


def kernel(
    nkx, ncz, pieces,
    field_modes, cotangent, tables_in,
    out,
    raw, tables, raw_sem, table_sem, ready,
    wide, rows, held, mixed, parts, points, total, flux, lowered, turned, result, landed,
    in_send, in_recv, swap_send, swap_recv, back_send, back_recv, out_send, out_recv,
):
    local_k, fields, columns = field_modes.shape
    rows_y = rows.shape[1]
    local_m = columns // rows_y
    own_rows = rows_y // nkx
    points_x = local_m * nkx
    points_z = points.shape[2]
    modes_z = local_k * ncz
    share_x = points_x // ncz
    aligned = local_k % 128 == 0
    i, j = lax.axis_index("kx"), lax.axis_index("cz")
    ahead = 3
    order = ((0, 2), (1, 0), (1, 1), (1, 3), (0, 0), (0, 1), (0, 3), (1, 2))

    places = nkx // 2
    place, column = i // 2, lax.rem(i, 2)
    above, below = place + 1 < places, place > 0
    inner = jnp.logical_or(place == places // 2 - 1, place == places // 2)
    near = 1 + jnp.where(above, 1, 0) + jnp.where(below, 1, 0)

    def at(row_owner, mode_owner):
        return {"kx": row_owner, "cz": mode_owner}

    def wait(ref, sem):
        pltpu.make_async_copy(ref, ref, sem).wait()

    piece = columns // pieces
    raw_copies = [
        [
            pltpu.make_async_copy(
                array.at[:, :, pl.ds(p * piece, piece)], raw.at[a, :, :, pl.ds(p * piece, piece)], raw_sem.at[a, p]
            )
            for p in range(pieces)
        ]
        for a, array in enumerate((field_modes, cotangent))
    ]
    table_copy = pltpu.make_async_copy(tables_in, tables, table_sem)
    for copy in raw_copies[0]:
        copy.start()
    barrier = pltpu.get_barrier_semaphore()

    def signal_near(sem):
        pl.semaphore_signal(sem, inc=1, device_id=at(place * 2 + 1 - column, j), device_id_type=MESH)

        @pl.when(above)
        def _():
            pl.semaphore_signal(sem, inc=1, device_id=at(i + 2, j), device_id_type=MESH)

        @pl.when(below)
        def _():
            pl.semaphore_signal(sem, inc=1, device_id=at(i - 2, j), device_id_type=MESH)

    signal_near(barrier)
    for step in range(1, ncz):
        pl.semaphore_signal(barrier, inc=1, device_id=at(i, lax.rem(j + step, ncz)), device_id_type=MESH)
    for copy in raw_copies[1]:
        copy.start()

    hartley = tables.at[pl.ds(0, points_x)]
    lifts = [tables.at[pl.ds(points_x + n * modes_z, modes_z)] for n in range(2)]
    chunk = 128 if piece % 128 == 0 else piece

    def prepare(h):
        a, f = order[h]

        def turn(step, carry):
            here = pl.ds(pl.multiple_of(step * chunk, chunk), chunk)
            wide[here, :] = raw[a, :, f, here].astype(jnp.float32).T
            return carry

        for p in range(pieces):
            if h < 2:
                raw_copies[a][p].wait()
                lax.fori_loop(p * (piece // chunk), (p + 1) * (piece // chunk), turn, 0)
        if h >= 2:
            lax.fori_loop(0, columns // chunk, turn, 0)
        for y in range(rows_y):
            rows[h, y] = wide[pl.ds(y, local_m, stride=rows_y), :].astype(jnp.bfloat16)

    def in_place(h):
        return held.at[h, :, pl.ds(pl.multiple_of(i * local_m, local_m), local_m)]

    def send_in(h, target):
        pltpu.make_async_remote_copy(
            src_ref=rows.at[h, pl.ds(target * own_rows, own_rows)],
            dst_ref=in_place(h),
            send_sem=in_send,
            recv_sem=in_recv.at[h],
            device_id=at(target, j),
            device_id_type=MESH,
        ).start()

    def keep_in(h):
        pltpu.make_async_copy(rows.at[h, pl.ds(i * own_rows, own_rows)], in_place(h), in_recv.at[h]).start()

    def flip(index, step):
        bit = 1
        target = index
        while bit < nkx:
            if step & bit:
                target = target + bit * (1 - 2 * lax.rem(index // bit, 2))
            bit *= 2
        return target

    half = nkx // 2
    within = list(range(1, half))
    across = [s for s in range(half, nkx) if s % 2] + [s for s in range(half, nkx) if not s % 2]

    def targets(chosen):
        if nkx & (nkx - 1):
            return [lax.rem(i + s, nkx) for s in chosen]
        return [flip(i, s) for s in chosen]

    def send_at_distance(h, distance):
        for hops, side in ((distance, 0), (distance - 1, 1)):
            facing = place * 2 + (column if side == 0 else 1 - column)
            if hops == 0:
                send_in(h, facing)
            elif hops < places:
                @pl.when(place + hops < places)
                def _():
                    send_in(h, facing + 2 * hops)

                @pl.when(place >= hops)
                def _():
                    send_in(h, facing - 2 * hops)

    prepare(0)
    pl.semaphore_wait(barrier, near + ncz - 1)
    send_at_distance(0, 1)
    for distance in range(2, places + 1):
        sem = ready.at[distance - 2]
        signal_near(sem)
        pl.semaphore_wait(sem, near)
        send_at_distance(0, distance)
    keep_in(0)
    table_copy.start()

    def launch(h):
        if h < 2 * fields:
            prepare(h)
            for target in targets(within + across):
                send_in(h, target)
            keep_in(h)

    for h in range(1, ahead):
        launch(h)

    def share_rows(q):
        return pl.ds(pl.multiple_of(q * share_x, share_x), share_x)

    def lanes(r):
        return slice(r * local_k, (r + 1) * local_k)

    def transform(target, source):
        if aligned:
            joined = source[0] if len(source) == 1 else jnp.concatenate(source, axis=1)
            value = matmul(hartley[...], joined).astype(jnp.bfloat16)
            for r in range(own_rows):
                target(r, value[:, lanes(r)])
        else:
            for r in range(own_rows):
                target(r, matmul(hartley[...], source[r]).astype(jnp.bfloat16))

    def mix(h):
        wait(held.at[h], in_recv.at[h])

        def keep(r, value):
            mixed[h, :, lanes(r)] = value

        transform(keep, [held[h, r] for r in range(own_rows)])
        for step in range(1, ncz):
            q = lax.rem(j + step, ncz)
            pltpu.make_async_remote_copy(
                src_ref=mixed.at[h, share_rows(q), :],
                dst_ref=parts.at[h, j],
                send_sem=swap_send,
                recv_sem=swap_recv.at[h],
                device_id=at(i, q),
                device_id_type=MESH,
            ).start()
        pltpu.make_async_copy(mixed.at[h, share_rows(j), :], parts.at[h, j], swap_recv.at[h]).start()

    block_z = 256 if points_z % 256 == 0 else points_z

    def lift(h, use):
        wait(parts.at[h], swap_recv.at[h])
        table = lifts[order[h][0]]

        def one(step, carry):
            here = pl.ds(pl.multiple_of(step * block_z, block_z), block_z)
            if aligned:
                joined = jnp.concatenate(
                    [
                        jnp.concatenate([parts[h, q, :, lanes(r)] for q in range(ncz)], axis=1)
                        for r in range(own_rows)
                    ],
                    axis=0,
                )
                use(slice(None), here, matmul(joined, table[:, here]))
            else:
                for r in range(own_rows):
                    value = matmul(parts[h, 0, :, lanes(r)], table[0:local_k, here])
                    for q in range(1, ncz):
                        value += matmul(parts[h, q, :, lanes(r)], table[q * local_k:(q + 1) * local_k, here])
                    use(slice(r * share_x, (r + 1) * share_x), here, value)
            return carry

        lax.fori_loop(0, points_z // block_z, one, 0)

    def leave(f):
        if aligned:
            value = matmul_t(flux[...], lifts[0][...]).astype(jnp.bfloat16)
            for q in range(ncz):
                for r in range(own_rows):
                    lowered[f, q, :, lanes(r)] = value[r * share_x:(r + 1) * share_x, lanes(q)]
        else:
            for q in range(ncz):
                for r in range(own_rows):
                    lowered[f, q, :, lanes(r)] = matmul_t(
                        flux[r * share_x:(r + 1) * share_x, :], lifts[0][q * local_k:(q + 1) * local_k, :]
                    ).astype(jnp.bfloat16)
        for step in range(1, ncz):
            q = lax.rem(j + step, ncz)
            pltpu.make_async_remote_copy(
                src_ref=lowered.at[f, q],
                dst_ref=turned.at[f, share_rows(j), :],
                send_sem=back_send,
                recv_sem=back_recv.at[f],
                device_id=at(i, q),
                device_id_type=MESH,
            ).start()
        pltpu.make_async_copy(lowered.at[f, j], turned.at[f, share_rows(j), :], back_recv.at[f]).start()

    def out_block(f, target):
        return result.at[f, :, pl.ds(pl.multiple_of(target * local_m, local_m), local_m)]

    def out_place(f):
        return landed.at[f, pl.ds(i * own_rows, own_rows)]

    def finish(f):
        wait(turned.at[f], back_recv.at[f])

        def keep(r, value):
            result[f, r] = value

        transform(keep, [turned[f, :, lanes(r)] for r in range(own_rows)])
        pltpu.make_async_copy(out_block(f, i), out_place(f), out_recv.at[f]).start()

    def depart(f, chosen):
        for target in targets(chosen):
            pltpu.make_async_remote_copy(
                src_ref=out_block(f, target),
                dst_ref=out_place(f),
                send_sem=out_send,
                recv_sem=out_recv.at[f],
                device_id=at(target, j),
                device_id_type=MESH,
            ).start()

    outer = jnp.logical_not(inner)

    def keep(h):
        def use(part, here, value):
            points[h, part, here] = value
        return use

    def keep_and_flux(h):
        def use(part, here, value):
            points[h, part, here] = value
            flux[part, here] = (value * points[0, part, here]).astype(jnp.bfloat16)
        return use

    def first(part, here, value):
        total[part, here] = points[1, part, here] * value

    def add(h):
        def use(part, here, value):
            total[part, here] += points[h, part, here] * value
        return use

    def last(part, here, value):
        flux[part, here] = (total[part, here] + 2.0 * value * points[0, part, here]).astype(jnp.bfloat16)

    table_copy.wait()
    mix(0)
    launch(ahead)
    mix(1)
    launch(ahead + 1)
    lift(0, keep(0))
    mix(2)
    launch(ahead + 2)
    lift(1, keep_and_flux(1))
    leave(0)
    mix(3)
    launch(ahead + 3)
    lift(2, keep_and_flux(2))
    leave(1)
    finish(0)
    mix(4)
    launch(ahead + 4)
    lift(3, keep_and_flux(3))
    leave(3)
    finish(1)

    @pl.when(inner)
    def _():
        depart(0, within + across)
        depart(1, within + across)

    mix(5)
    launch(ahead + 5)
    lift(4, first)
    finish(3)

    @pl.when(inner)
    def _():
        depart(3, within + across)

    mix(6)
    launch(ahead + 6)
    lift(5, add(2))
    mix(7)

    @pl.when(outer)
    def _():
        for f in (0, 1, 3):
            depart(f, within + across)

    lift(6, add(3))
    lift(7, last)
    leave(2)
    finish(2)
    depart(2, within + across)

    for f in (0, 1, 3, 2):
        wait(landed.at[f], out_recv.at[f])
        for y in range(rows_y):
            wide[pl.ds(y, local_m, stride=rows_y), :] = landed[f, y].astype(jnp.float32)

        def settle(step, carry):
            here = pl.ds(pl.multiple_of(step * chunk, chunk), chunk)
            out[f, here, :] = wide[here, :].astype(jnp.bfloat16)
            return carry

        lax.fori_loop(0, columns // chunk, settle, 0)

    wait(rows.at[:, pl.ds(0, rows_y - own_rows)], in_send)
    wait(mixed.at[:, pl.ds(0, points_x - share_x), :], swap_send)
    wait(lowered.at[:, pl.ds(0, ncz - 1)], back_send)
    wait(landed.at[:, pl.ds(0, rows_y - own_rows)], out_send)


def on_device(nkx, ncz, field_modes, cotangent):
    local_k, fields, columns = field_modes.shape
    local_m = columns // Y
    modes_z, points_x = local_k * ncz, local_m * nkx
    own_rows = Y // nkx
    share_x = points_x // ncz
    bf16 = jnp.bfloat16
    pieces = next(p for p in (4, 3, 2, 1) if columns % (p * 128) == 0 or p == 1)

    cosines = cosine_table(MZ, modes_z)
    synthesis = (cosines * math.sqrt(2.0 / modes_z)).astype(bf16).T
    projection = (cosines * math.sqrt(2.0 / MZ)).astype(bf16).T
    hartley = hartley_table(points_x).astype(np.float32).astype(bf16)
    tables = jnp.asarray(np.concatenate([hartley, synthesis, projection], axis=0))

    hbm = pl.BlockSpec(memory_space=pltpu.HBM)
    dma = pltpu.SemaphoreType.DMA
    out = pl.pallas_call(
        functools.partial(kernel, nkx, ncz, pieces),
        out_shape=jax.ShapeDtypeStruct((fields, columns, local_k), bf16),
        in_specs=[hbm] * 3,
        out_specs=pl.BlockSpec(memory_space=pltpu.VMEM),
        scratch_shapes=[
            pltpu.VMEM((2, local_k, fields, columns), bf16),
            pltpu.VMEM(tables.shape, bf16),
            dma((2, pieces)), dma, pltpu.SemaphoreType.REGULAR((nkx // 2,)),
            pltpu.VMEM((columns, local_k), jnp.float32),
            pltpu.VMEM((2 * fields, Y, local_m, local_k), bf16),
            pltpu.VMEM((2 * fields, own_rows, points_x, local_k), bf16),
            pltpu.VMEM((2 * fields, points_x, own_rows * local_k), bf16),
            pltpu.VMEM((2 * fields, ncz, share_x, own_rows * local_k), bf16),
            pltpu.VMEM((fields, own_rows * share_x, MZ), jnp.float32),
            pltpu.VMEM((own_rows * share_x, MZ), jnp.float32),
            pltpu.VMEM((own_rows * share_x, MZ), bf16),
            pltpu.VMEM((fields, ncz, share_x, own_rows * local_k), bf16),
            pltpu.VMEM((fields, points_x, own_rows * local_k), bf16),
            pltpu.VMEM((fields, own_rows, points_x, local_k), bf16),
            pltpu.VMEM((fields, Y, local_m, local_k), bf16),
            dma, dma((2 * fields,)), dma, dma((2 * fields,)),
            dma, dma((fields,)), dma, dma((fields,)),
        ],
        compiler_params=pltpu.CompilerParams(has_side_effects=True, vmem_limit_bytes=52 * 2**20, collective_id=0),
    )(field_modes, cotangent, tables)
    return out.transpose(2, 0, 1)


def solution(mesh):
    return jax.shard_map(
        functools.partial(on_device, mesh.shape["kx"], mesh.shape["cz"]),
        mesh=mesh,
        in_specs=(P("cz", None, "kx"), P("cz", None, "kx")),
        out_specs=P("cz", None, "kx"),
        check_vma=False,
    )
```

```python
import functools
import math

import jax
import jax.numpy as jnp
import numpy as np
from jax import lax
from jax.experimental import pallas as pl
from jax.experimental.pallas import tpu as pltpu
from jax.sharding import PartitionSpec as P

MZ = 768
Y = 16
MESH = pl.DeviceIdType.MESH


def cosine_table(rows, columns):
    position = (np.arange(columns)[None, :] * (2 * np.arange(rows)[:, None] + 1)) % (4 * rows)
    return np.cos(np.pi * position / (2 * rows)).astype(np.float32)


def hartley_table(points):
    index = np.arange(points)
    phases = 2.0 * np.pi * ((index[:, None] * index[None, :]) % points) / points
    return (np.cos(phases) + np.sin(phases)) / math.sqrt(points)


def matmul(a, b):
    return jnp.dot(a, b, preferred_element_type=jnp.float32)


def matmul_t(a, b):
    return lax.dot_general(a, b, (((1,), (1,)), ((), ())), preferred_element_type=jnp.float32)


def kernel(
    nkx, ncz, pieces,
    field_modes, cotangent, tables_in,
    out,
    raw, tables, raw_sem, table_sem, ready,
    weave, wide, rows, held, mixed, parts, points, total, flux, lowered, turned, result, landed,
    in_send, in_recv, swap_send, swap_recv, back_send, back_recv, out_send, out_recv,
):
    local_k, fields, columns = field_modes.shape
    rows_y = rows.shape[1]
    local_m = columns // rows_y
    own_rows = rows_y // nkx
    points_x = local_m * nkx
    points_z = points.shape[2]
    modes_z = local_k * ncz
    share_x = points_x // ncz
    aligned = local_k % 128 == 0
    i, j = lax.axis_index("kx"), lax.axis_index("cz")
    ahead = 3
    order = ((0, 2), (1, 0), (1, 1), (1, 3), (0, 0), (0, 1), (0, 3), (1, 2))

    places = nkx // 2
    place, column = i // 2, lax.rem(i, 2)
    above, below = place + 1 < places, place > 0
    inner = jnp.logical_or(place == places // 2 - 1, place == places // 2)
    near = 1 + jnp.where(above, 1, 0) + jnp.where(below, 1, 0)

    def at(row_owner, mode_owner):
        return {"kx": row_owner, "cz": mode_owner}

    def wait(ref, sem):
        pltpu.make_async_copy(ref, ref, sem).wait()

    piece = columns // pieces
    raw_copies = [
        [
            pltpu.make_async_copy(
                array.at[:, :, pl.ds(p * piece, piece)], raw.at[a, :, :, pl.ds(p * piece, piece)], raw_sem.at[a, p]
            )
            for p in range(pieces)
        ]
        for a, array in enumerate((field_modes, cotangent))
    ]
    table_copy = pltpu.make_async_copy(tables_in, tables, table_sem)
    for copy in raw_copies[0]:
        copy.start()
    barrier = pltpu.get_barrier_semaphore()

    def signal_near(sem):
        pl.semaphore_signal(sem, inc=1, device_id=at(place * 2 + 1 - column, j), device_id_type=MESH)

        @pl.when(above)
        def _():
            pl.semaphore_signal(sem, inc=1, device_id=at(i + 2, j), device_id_type=MESH)

        @pl.when(below)
        def _():
            pl.semaphore_signal(sem, inc=1, device_id=at(i - 2, j), device_id_type=MESH)

    signal_near(barrier)
    for step in range(1, ncz):
        pl.semaphore_signal(barrier, inc=1, device_id=at(i, lax.rem(j + step, ncz)), device_id_type=MESH)

    hartley = tables.at[pl.ds(0, points_x)]
    lifts = [tables.at[pl.ds(points_x + n * modes_z, modes_z)] for n in range(2)]
    group = 16
    block = group * rows_y
    row = lax.broadcasted_iota(jnp.int32, (block, block), 0)
    lane = lax.broadcasted_iota(jnp.int32, (block, block), 1)
    moved = lax.rem(row, group) * rows_y + row // group
    weave[...] = jnp.where(moved == lane, 1.0, 0.0).astype(jnp.bfloat16)

    def prepare(h, between=None):
        a, f = order[h]

        def turn(step, carry):
            here = pl.ds(pl.multiple_of(step * block, block), block)
            value = matmul_t(weave[...], raw[a, :, f, here]).astype(jnp.bfloat16)
            rows[h, :, pl.ds(pl.multiple_of(step * group, group), group), :] = value.reshape(rows_y, group, local_k)
            return carry

        if h >= 2:
            lax.fori_loop(0, columns // block, turn, 0)
        else:
            span = columns // block // pieces
            for p in range(pieces):
                raw_copies[a][p].wait()
                lax.fori_loop(p * span, (p + 1) * span, turn, 0)
                if between is not None:
                    between(p)

    def in_place(h, start=0, count=local_m):
        return held.at[h, :, pl.ds(pl.multiple_of(i * local_m, local_m) + start, count)]

    def send_in(h, target, start=0, count=local_m):
        pltpu.make_async_remote_copy(
            src_ref=rows.at[h, pl.ds(target * own_rows, own_rows), pl.ds(start, count)],
            dst_ref=in_place(h, start, count),
            send_sem=in_send,
            recv_sem=in_recv.at[h],
            device_id=at(target, j),
            device_id_type=MESH,
        ).start()

    def keep_in(h):
        pltpu.make_async_copy(rows.at[h, pl.ds(i * own_rows, own_rows)], in_place(h), in_recv.at[h]).start()

    def flip(index, step):
        bit = 1
        target = index
        while bit < nkx:
            if step & bit:
                target = target + bit * (1 - 2 * lax.rem(index // bit, 2))
            bit *= 2
        return target

    half = nkx // 2
    within = list(range(1, half))
    across = [s for p in range(half // 2, places) for s in (2 * p + 1, 2 * p)]

    def targets(chosen):
        if nkx & (nkx - 1):
            return [lax.rem(i + s, nkx) for s in chosen]
        return [flip(i, s) for s in chosen]

    def send_at_distance(h, distance, start=0, count=local_m):
        for hops, side in ((distance, 0), (distance - 1, 1)):
            facing = place * 2 + (column if side == 0 else 1 - column)
            if hops == 0:
                send_in(h, facing, start, count)
            elif hops < places:
                @pl.when(place + hops < places)
                def _():
                    send_in(h, facing + 2 * hops, start, count)

                @pl.when(place >= hops)
                def _():
                    send_in(h, facing - 2 * hops, start, count)

    part_m = local_m // pieces

    def begin(p):
        if p == 0:
            pl.semaphore_wait(barrier, near + ncz - 1)
            if places > 1:
                signal_near(ready.at[0])
        if p == pieces - 1:
            for copy in raw_copies[1]:
                copy.start()
        send_at_distance(0, 1, p * part_m, part_m)

    prepare(0, begin)
    for distance in range(2, places + 1):
        pl.semaphore_wait(ready.at[distance - 2], near)
        if distance < places:
            signal_near(ready.at[distance - 1])
        send_at_distance(0, distance)
    keep_in(0)
    table_copy.start()

    def launch(h):
        if h < 2 * fields:
            prepare(h)
            for target in targets(within + across):
                send_in(h, target)
            keep_in(h)

    for h in range(1, ahead):
        launch(h)

    def share_rows(q):
        return pl.ds(pl.multiple_of(q * share_x, share_x), share_x)

    def lanes(r):
        return slice(r * local_k, (r + 1) * local_k)

    def transform(target, source):
        if aligned:
            joined = source[0] if len(source) == 1 else jnp.concatenate(source, axis=1)
            value = matmul(hartley[...], joined).astype(jnp.bfloat16)
            for r in range(own_rows):
                target(r, value[:, lanes(r)])
        else:
            for r in range(own_rows):
                target(r, matmul(hartley[...], source[r]).astype(jnp.bfloat16))

    def mix(h):
        wait(held.at[h], in_recv.at[h])

        def keep(r, value):
            mixed[h, :, lanes(r)] = value

        transform(keep, [held[h, r] for r in range(own_rows)])
        for step in range(1, ncz):
            q = lax.rem(j + step, ncz)
            pltpu.make_async_remote_copy(
                src_ref=mixed.at[h, share_rows(q), :],
                dst_ref=parts.at[h, j],
                send_sem=swap_send,
                recv_sem=swap_recv.at[h],
                device_id=at(i, q),
                device_id_type=MESH,
            ).start()
        pltpu.make_async_copy(mixed.at[h, share_rows(j), :], parts.at[h, j], swap_recv.at[h]).start()

    block_z = 256 if points_z % 256 == 0 else points_z

    def lift(h, use):
        wait(parts.at[h], swap_recv.at[h])
        table = lifts[order[h][0]]

        def one(step, carry):
            here = pl.ds(pl.multiple_of(step * block_z, block_z), block_z)
            if aligned:
                joined = jnp.concatenate(
                    [
                        jnp.concatenate([parts[h, q, :, lanes(r)] for q in range(ncz)], axis=1)
                        for r in range(own_rows)
                    ],
                    axis=0,
                )
                use(slice(None), here, matmul(joined, table[:, here]))
            else:
                for r in range(own_rows):
                    value = matmul(parts[h, 0, :, lanes(r)], table[0:local_k, here])
                    for q in range(1, ncz):
                        value += matmul(parts[h, q, :, lanes(r)], table[q * local_k:(q + 1) * local_k, here])
                    use(slice(r * share_x, (r + 1) * share_x), here, value)
            return carry

        lax.fori_loop(0, points_z // block_z, one, 0)

    def leave(f):
        if aligned:
            value = matmul_t(flux[...], lifts[0][...]).astype(jnp.bfloat16)
            for q in range(ncz):
                for r in range(own_rows):
                    lowered[f, q, :, lanes(r)] = value[r * share_x:(r + 1) * share_x, lanes(q)]
        else:
            for q in range(ncz):
                for r in range(own_rows):
                    lowered[f, q, :, lanes(r)] = matmul_t(
                        flux[r * share_x:(r + 1) * share_x, :], lifts[0][q * local_k:(q + 1) * local_k, :]
                    ).astype(jnp.bfloat16)
        for step in range(1, ncz):
            q = lax.rem(j + step, ncz)
            pltpu.make_async_remote_copy(
                src_ref=lowered.at[f, q],
                dst_ref=turned.at[f, share_rows(j), :],
                send_sem=back_send,
                recv_sem=back_recv.at[f],
                device_id=at(i, q),
                device_id_type=MESH,
            ).start()
        pltpu.make_async_copy(lowered.at[f, j], turned.at[f, share_rows(j), :], back_recv.at[f]).start()

    def out_block(f, target):
        return result.at[f, :, pl.ds(pl.multiple_of(target * local_m, local_m), local_m)]

    def out_place(f):
        return landed.at[f, pl.ds(i * own_rows, own_rows)]

    def finish(f):
        wait(turned.at[f], back_recv.at[f])

        def keep(r, value):
            result[f, r] = value

        transform(keep, [turned[f, :, lanes(r)] for r in range(own_rows)])
        pltpu.make_async_copy(out_block(f, i), out_place(f), out_recv.at[f, i]).start()

    def depart(f, chosen):
        for target in targets(chosen):
            pltpu.make_async_remote_copy(
                src_ref=out_block(f, target),
                dst_ref=out_place(f),
                send_sem=out_send,
                recv_sem=out_recv.at[f, i],
                device_id=at(target, j),
                device_id_type=MESH,
            ).start()

    outer = jnp.logical_not(inner)

    def keep(h):
        def use(part, here, value):
            points[h, part, here] = value
        return use

    def keep_and_flux(h):
        def use(part, here, value):
            points[h, part, here] = value
            flux[part, here] = (value * points[0, part, here]).astype(jnp.bfloat16)
        return use

    def first(part, here, value):
        total[part, here] = points[1, part, here] * value

    def add(h):
        def use(part, here, value):
            total[part, here] += points[h, part, here] * value
        return use

    def last(part, here, value):
        flux[part, here] = (total[part, here] + 2.0 * value * points[0, part, here]).astype(jnp.bfloat16)

    table_copy.wait()
    mix(0)
    launch(ahead)
    mix(1)
    launch(ahead + 1)
    lift(0, keep(0))
    mix(2)
    launch(ahead + 2)
    lift(1, keep_and_flux(1))
    leave(0)
    mix(3)
    launch(ahead + 3)
    lift(2, keep_and_flux(2))
    leave(1)
    finish(0)
    mix(4)
    launch(ahead + 4)
    lift(3, keep_and_flux(3))
    leave(3)
    finish(1)

    @pl.when(inner)
    def _():
        depart(0, within + across)
        depart(1, within + across)

    mix(5)
    launch(ahead + 5)
    lift(4, first)
    finish(3)

    @pl.when(inner)
    def _():
        depart(3, within + across)

    mix(6)
    launch(ahead + 6)
    lift(5, add(2))
    mix(7)

    @pl.when(outer)
    def _():
        for f in (0, 1, 3):
            depart(f, within + across)

    lift(6, add(3))
    lift(7, last)
    leave(2)
    finish(2)
    depart(2, within + across)

    chunk = 128 if columns % 128 == 0 else columns
    for f in (0, 1, 3, 2):
        for step in [0] + within + across:
            source = targets([step])[0]
            wait(landed.at[f, pl.ds(source * own_rows, own_rows)], out_recv.at[f, source])
            for r in range(own_rows):
                y = source * own_rows + r
                wide[pl.ds(y, local_m, stride=rows_y), :] = landed[f, y].astype(jnp.float32)

        def settle(step, carry):
            here = pl.ds(pl.multiple_of(step * chunk, chunk), chunk)
            out[f, here, :] = wide[here, :].astype(jnp.bfloat16)
            return carry

        lax.fori_loop(0, columns // chunk, settle, 0)

    wait(rows.at[:, pl.ds(0, rows_y - own_rows)], in_send)
    wait(mixed.at[:, pl.ds(0, points_x - share_x), :], swap_send)
    wait(lowered.at[:, pl.ds(0, ncz - 1)], back_send)
    wait(landed.at[:, pl.ds(0, rows_y - own_rows)], out_send)


def on_device(nkx, ncz, field_modes, cotangent):
    local_k, fields, columns = field_modes.shape
    local_m = columns // Y
    modes_z, points_x = local_k * ncz, local_m * nkx
    own_rows = Y // nkx
    share_x = points_x // ncz
    bf16 = jnp.bfloat16
    pieces = next(p for p in (3, 2, 1) if columns % (p * 16 * Y) == 0 or p == 1)

    cosines = cosine_table(MZ, modes_z)
    synthesis = (cosines * math.sqrt(2.0 / modes_z)).astype(bf16).T
    projection = (cosines * math.sqrt(2.0 / MZ)).astype(bf16).T
    hartley = hartley_table(points_x).astype(np.float32).astype(bf16)
    tables = jnp.asarray(np.concatenate([hartley, synthesis, projection], axis=0))

    hbm = pl.BlockSpec(memory_space=pltpu.HBM)
    dma = pltpu.SemaphoreType.DMA
    out = pl.pallas_call(
        functools.partial(kernel, nkx, ncz, pieces),
        out_shape=jax.ShapeDtypeStruct((fields, columns, local_k), bf16),
        in_specs=[hbm] * 3,
        out_specs=pl.BlockSpec(memory_space=pltpu.VMEM),
        scratch_shapes=[
            pltpu.VMEM((2, local_k, fields, columns), bf16),
            pltpu.VMEM(tables.shape, bf16),
            dma((2, pieces)), dma, pltpu.SemaphoreType.REGULAR((nkx // 2,)),
            pltpu.VMEM((16 * Y, 16 * Y), bf16),
            pltpu.VMEM((columns, local_k), jnp.float32),
            pltpu.VMEM((2 * fields, Y, local_m, local_k), bf16),
            pltpu.VMEM((2 * fields, own_rows, points_x, local_k), bf16),
            pltpu.VMEM((2 * fields, points_x, own_rows * local_k), bf16),
            pltpu.VMEM((2 * fields, ncz, share_x, own_rows * local_k), bf16),
            pltpu.VMEM((fields, own_rows * share_x, MZ), jnp.float32),
            pltpu.VMEM((own_rows * share_x, MZ), jnp.float32),
            pltpu.VMEM((own_rows * share_x, MZ), bf16),
            pltpu.VMEM((fields, ncz, share_x, own_rows * local_k), bf16),
            pltpu.VMEM((fields, points_x, own_rows * local_k), bf16),
            pltpu.VMEM((fields, own_rows, points_x, local_k), bf16),
            pltpu.VMEM((fields, Y, local_m, local_k), bf16),
            dma, dma((2 * fields,)), dma, dma((2 * fields,)),
            dma, dma((fields,)), dma, dma((fields, nkx)),
        ],
        compiler_params=pltpu.CompilerParams(has_side_effects=True, vmem_limit_bytes=52 * 2**20, collective_id=0),
    )(field_modes, cotangent, tables)
    return out.transpose(2, 0, 1)


def solution(mesh):
    return jax.shard_map(
        functools.partial(on_device, mesh.shape["kx"], mesh.shape["cz"]),
        mesh=mesh,
        in_specs=(P("cz", None, "kx"), P("cz", None, "kx")),
        out_specs=P("cz", None, "kx"),
        check_vma=False,
    )
```

```python
import functools
import math

import jax
import jax.numpy as jnp
import numpy as np
from jax import lax
from jax.experimental import pallas as pl
from jax.experimental.pallas import tpu as pltpu
from jax.sharding import PartitionSpec as P

MZ = 768
Y = 16
MESH = pl.DeviceIdType.MESH


def cosine_table(rows, columns):
    position = (np.arange(columns)[None, :] * (2 * np.arange(rows)[:, None] + 1)) % (4 * rows)
    return np.cos(np.pi * position / (2 * rows)).astype(np.float32)


def hartley_table(points):
    index = np.arange(points)
    phases = 2.0 * np.pi * ((index[:, None] * index[None, :]) % points) / points
    return (np.cos(phases) + np.sin(phases)) / math.sqrt(points)


def matmul(a, b):
    return jnp.dot(a, b, preferred_element_type=jnp.float32)


def matmul_t(a, b):
    return lax.dot_general(a, b, (((1,), (1,)), ((), ())), preferred_element_type=jnp.float32)


def kernel(
    nkx, ncz, pieces,
    field_modes, cotangent, tables_in,
    out,
    raw, tables, raw_sem, table_sem, ready,
    weave, wide, stage, rows, held, mixed, parts, points, total, flux, lowered, turned, result, landed,
    in_send, in_recv, swap_send, swap_recv, back_send, back_recv, out_send, out_recv,
):
    local_k, fields, columns = field_modes.shape
    rows_y = rows.shape[1]
    local_m = columns // rows_y
    own_rows = rows_y // nkx
    points_x = local_m * nkx
    points_z = points.shape[2]
    modes_z = local_k * ncz
    share_x = points_x // ncz
    aligned = local_k % 128 == 0
    i, j = lax.axis_index("kx"), lax.axis_index("cz")
    ahead = 3
    order = ((0, 2), (1, 0), (1, 1), (1, 3), (0, 0), (0, 1), (0, 3), (1, 2))

    places = nkx // 2
    place, column = i // 2, lax.rem(i, 2)
    above, below = place + 1 < places, place > 0
    inner = jnp.logical_or(place == places // 2 - 1, place == places // 2)
    near = 1 + jnp.where(above, 1, 0) + jnp.where(below, 1, 0)

    def at(row_owner, mode_owner):
        return {"kx": row_owner, "cz": mode_owner}

    def wait(ref, sem):
        pltpu.make_async_copy(ref, ref, sem).wait()

    piece = columns // pieces
    raw_copies = [
        [
            pltpu.make_async_copy(
                array.at[:, :, pl.ds(p * piece, piece)], raw.at[a, :, :, pl.ds(p * piece, piece)], raw_sem.at[a, p]
            )
            for p in range(pieces)
        ]
        for a, array in enumerate((field_modes, cotangent))
    ]
    table_copy = pltpu.make_async_copy(tables_in, tables, table_sem)
    for copy in raw_copies[0]:
        copy.start()
    barrier = pltpu.get_barrier_semaphore()

    def signal_near(sem):
        pl.semaphore_signal(sem, inc=1, device_id=at(place * 2 + 1 - column, j), device_id_type=MESH)

        @pl.when(above)
        def _():
            pl.semaphore_signal(sem, inc=1, device_id=at(i + 2, j), device_id_type=MESH)

        @pl.when(below)
        def _():
            pl.semaphore_signal(sem, inc=1, device_id=at(i - 2, j), device_id_type=MESH)

    signal_near(barrier)
    for step in range(1, ncz):
        pl.semaphore_signal(barrier, inc=1, device_id=at(i, lax.rem(j + step, ncz)), device_id_type=MESH)

    hartley = tables.at[pl.ds(0, points_x)]
    lifts = [tables.at[pl.ds(points_x + n * modes_z, modes_z)] for n in range(2)]
    chunk, group = 128, 16
    block = group * rows_y
    row = lax.broadcasted_iota(jnp.int32, (block, block), 0)
    lane = lax.broadcasted_iota(jnp.int32, (block, block), 1)
    moved = lax.rem(row, group) * rows_y + row // group
    weave[...] = jnp.where(moved == lane, 1.0, 0.0).astype(jnp.bfloat16)

    def prepare(h, between=None):
        a, f = order[h]

        def turn(step, carry):
            here = pl.ds(pl.multiple_of(step * block, block), block)
            value = matmul_t(weave[...], raw[a, :, f, here]).astype(jnp.bfloat16)
            rows[h, :, pl.ds(pl.multiple_of(step * group, group), group), :] = value.reshape(rows_y, group, local_k)
            return carry

        if h >= 2:
            lax.fori_loop(0, columns // block, turn, 0)
        else:
            span = columns // block // pieces
            for p in range(pieces):
                raw_copies[a][p].wait()
                lax.fori_loop(p * span, (p + 1) * span, turn, 0)
                if between is not None:
                    between(p)

    def in_place(h, start=0, count=local_m):
        return held.at[h, :, pl.ds(pl.multiple_of(i * local_m, local_m) + start, count)]

    def send_in(h, target, start=0, count=local_m):
        pltpu.make_async_remote_copy(
            src_ref=rows.at[h, pl.ds(target * own_rows, own_rows), pl.ds(start, count)],
            dst_ref=in_place(h, start, count),
            send_sem=in_send,
            recv_sem=in_recv.at[h],
            device_id=at(target, j),
            device_id_type=MESH,
        ).start()

    def keep_in(h):
        pltpu.make_async_copy(rows.at[h, pl.ds(i * own_rows, own_rows)], in_place(h), in_recv.at[h]).start()

    def flip(index, step):
        bit = 1
        target = index
        while bit < nkx:
            if step & bit:
                target = target + bit * (1 - 2 * lax.rem(index // bit, 2))
            bit *= 2
        return target

    half = nkx // 2
    within = list(range(1, half))
    across = [s for p in range(half // 2, places) for s in (2 * p + 1, 2 * p)]

    def targets(chosen):
        if nkx & (nkx - 1):
            return [lax.rem(i + s, nkx) for s in chosen]
        return [flip(i, s) for s in chosen]

    def send_at_distance(h, distance, start=0, count=local_m):
        for hops, side in ((distance, 0), (distance - 1, 1)):
            facing = place * 2 + (column if side == 0 else 1 - column)
            if hops == 0:
                send_in(h, facing, start, count)
            elif hops < places:
                @pl.when(place + hops < places)
                def _():
                    send_in(h, facing + 2 * hops, start, count)

                @pl.when(place >= hops)
                def _():
                    send_in(h, facing - 2 * hops, start, count)

    part_m = local_m // pieces

    def begin(p):
        if p == 0:
            pl.semaphore_wait(barrier, near + ncz - 1)
            if places > 1:
                signal_near(ready.at[0])
        if p == pieces - 1:
            for copy in raw_copies[1]:
                copy.start()
        send_at_distance(0, 1, p * part_m, part_m)

    prepare(0, begin)
    for distance in range(2, places + 1):
        pl.semaphore_wait(ready.at[distance - 2], near)
        if distance < places:
            signal_near(ready.at[distance - 1])
        send_at_distance(0, distance)
    keep_in(0)
    table_copy.start()

    def launch(h):
        if h < 2 * fields:
            prepare(h)
            for target in targets(within + across):
                send_in(h, target)
            keep_in(h)

    for h in range(1, ahead):
        launch(h)

    def share_rows(q):
        return pl.ds(pl.multiple_of(q * share_x, share_x), share_x)

    def lanes(r):
        return slice(r * local_k, (r + 1) * local_k)

    def transform(target, source):
        if aligned:
            joined = source[0] if len(source) == 1 else jnp.concatenate(source, axis=1)
            value = matmul(hartley[...], joined).astype(jnp.bfloat16)
            for r in range(own_rows):
                target(r, value[:, lanes(r)])
        else:
            for r in range(own_rows):
                target(r, matmul(hartley[...], source[r]).astype(jnp.bfloat16))

    def mix(h):
        wait(held.at[h], in_recv.at[h])

        def keep(r, value):
            mixed[h, :, lanes(r)] = value

        transform(keep, [held[h, r] for r in range(own_rows)])
        for step in range(1, ncz):
            q = lax.rem(j + step, ncz)
            pltpu.make_async_remote_copy(
                src_ref=mixed.at[h, share_rows(q), :],
                dst_ref=parts.at[h, j],
                send_sem=swap_send,
                recv_sem=swap_recv.at[h],
                device_id=at(i, q),
                device_id_type=MESH,
            ).start()
        pltpu.make_async_copy(mixed.at[h, share_rows(j), :], parts.at[h, j], swap_recv.at[h]).start()

    block_z = 256 if points_z % 256 == 0 else points_z

    def lift(h, use):
        wait(parts.at[h], swap_recv.at[h])
        table = lifts[order[h][0]]

        def one(step, carry):
            here = pl.ds(pl.multiple_of(step * block_z, block_z), block_z)
            if aligned:
                joined = jnp.concatenate(
                    [
                        jnp.concatenate([parts[h, q, :, lanes(r)] for q in range(ncz)], axis=1)
                        for r in range(own_rows)
                    ],
                    axis=0,
                )
                use(slice(None), here, matmul(joined, table[:, here]))
            else:
                for r in range(own_rows):
                    value = matmul(parts[h, 0, :, lanes(r)], table[0:local_k, here])
                    for q in range(1, ncz):
                        value += matmul(parts[h, q, :, lanes(r)], table[q * local_k:(q + 1) * local_k, here])
                    use(slice(r * share_x, (r + 1) * share_x), here, value)
            return carry

        lax.fori_loop(0, points_z // block_z, one, 0)

    def leave(f):
        if aligned:
            value = matmul_t(flux[...], lifts[0][...]).astype(jnp.bfloat16)
            for q in range(ncz):
                for r in range(own_rows):
                    lowered[f, q, :, lanes(r)] = value[r * share_x:(r + 1) * share_x, lanes(q)]
        else:
            for q in range(ncz):
                for r in range(own_rows):
                    lowered[f, q, :, lanes(r)] = matmul_t(
                        flux[r * share_x:(r + 1) * share_x, :], lifts[0][q * local_k:(q + 1) * local_k, :]
                    ).astype(jnp.bfloat16)
        for step in range(1, ncz):
            q = lax.rem(j + step, ncz)
            pltpu.make_async_remote_copy(
                src_ref=lowered.at[f, q],
                dst_ref=turned.at[f, share_rows(j), :],
                send_sem=back_send,
                recv_sem=back_recv.at[f],
                device_id=at(i, q),
                device_id_type=MESH,
            ).start()
        pltpu.make_async_copy(lowered.at[f, j], turned.at[f, share_rows(j), :], back_recv.at[f]).start()

    def out_block(f, target):
        return result.at[f, :, pl.ds(pl.multiple_of(target * local_m, local_m), local_m)]

    def out_place(f):
        return landed.at[f, pl.ds(i * own_rows, own_rows)]

    def finish(f):
        wait(turned.at[f], back_recv.at[f])

        def keep(r, value):
            result[f, r] = value

        transform(keep, [turned[f, :, lanes(r)] for r in range(own_rows)])
        pltpu.make_async_copy(out_block(f, i), out_place(f), out_recv.at[f]).start()

    def depart(f, chosen):
        for target in targets(chosen):
            pltpu.make_async_remote_copy(
                src_ref=out_block(f, target),
                dst_ref=out_place(f),
                send_sem=out_send,
                recv_sem=out_recv.at[f],
                device_id=at(target, j),
                device_id_type=MESH,
            ).start()

    outer = jnp.logical_not(inner)

    def settle(f):
        wait(landed.at[f], out_recv.at[f])
        for y in range(rows_y):
            wide[pl.ds(y, local_m, stride=rows_y), :] = landed[f, y].astype(jnp.float32)

        def lay(step, carry):
            here = pl.ds(pl.multiple_of(step * chunk, chunk), chunk)
            stage[step, pl.ds(f, local_k, stride=fields), :] = wide[here, :].T
            if f == 2:
                out[step] = stage[step].astype(jnp.bfloat16)
            return carry

        lax.fori_loop(0, columns // chunk, lay, 0, unroll=f in (2, 3))

    def keep(h):
        def use(part, here, value):
            points[h, part, here] = value
        return use

    def keep_and_flux(h):
        def use(part, here, value):
            points[h, part, here] = value
            flux[part, here] = (value * points[0, part, here]).astype(jnp.bfloat16)
        return use

    def first(part, here, value):
        total[part, here] = points[1, part, here] * value

    def add(h):
        def use(part, here, value):
            total[part, here] += points[h, part, here] * value
        return use

    def last(part, here, value):
        flux[part, here] = (total[part, here] + 2.0 * value * points[0, part, here]).astype(jnp.bfloat16)

    table_copy.wait()
    mix(0)
    launch(ahead)
    mix(1)
    launch(ahead + 1)
    lift(0, keep(0))
    mix(2)
    launch(ahead + 2)
    lift(1, keep_and_flux(1))
    leave(0)
    mix(3)
    launch(ahead + 3)
    lift(2, keep_and_flux(2))
    leave(1)
    finish(0)
    mix(4)
    launch(ahead + 4)
    lift(3, keep_and_flux(3))
    leave(3)
    finish(1)

    @pl.when(inner)
    def _():
        depart(0, within + across)
        depart(1, within + across)

    mix(5)
    launch(ahead + 5)
    lift(4, first)
    finish(3)

    @pl.when(inner)
    def _():
        depart(3, within + across)

    mix(6)
    launch(ahead + 6)
    lift(5, add(2))
    mix(7)

    @pl.when(outer)
    def _():
        for f in (0, 1, 3):
            depart(f, within + across)

    lift(6, add(3))
    lift(7, last)
    leave(2)
    finish(2)
    depart(2, within + across)

    for f in (0, 1, 3, 2):
        settle(f)

    wait(rows.at[:, pl.ds(0, rows_y - own_rows)], in_send)
    wait(mixed.at[:, pl.ds(0, points_x - share_x), :], swap_send)
    wait(lowered.at[:, pl.ds(0, ncz - 1)], back_send)
    wait(landed.at[:, pl.ds(0, rows_y - own_rows)], out_send)


def deliver(tiles, out, sem):
    for n in range(tiles.shape[0]):
        pltpu.make_async_copy(tiles.at[n], out.at[:, :, pl.ds(n * 128, 128)], sem).start()
    pltpu.make_async_copy(out, out, sem).wait()


def on_device(nkx, ncz, field_modes, cotangent):
    local_k, fields, columns = field_modes.shape
    local_m = columns // Y
    modes_z, points_x = local_k * ncz, local_m * nkx
    own_rows = Y // nkx
    share_x = points_x // ncz
    bf16 = jnp.bfloat16
    pieces = next(p for p in (3, 2, 1) if columns % (p * 16 * Y) == 0 or p == 1)

    cosines = cosine_table(MZ, modes_z)
    synthesis = (cosines * math.sqrt(2.0 / modes_z)).astype(bf16).T
    projection = (cosines * math.sqrt(2.0 / MZ)).astype(bf16).T
    hartley = hartley_table(points_x).astype(np.float32).astype(bf16)
    tables = jnp.asarray(np.concatenate([hartley, synthesis, projection], axis=0))

    hbm = pl.BlockSpec(memory_space=pltpu.HBM)
    dma = pltpu.SemaphoreType.DMA
    out = pl.pallas_call(
        functools.partial(kernel, nkx, ncz, pieces),
        out_shape=jax.ShapeDtypeStruct((columns // 128, fields * local_k, 128), bf16),
        in_specs=[hbm] * 3,
        out_specs=pl.BlockSpec(memory_space=pltpu.VMEM),
        scratch_shapes=[
            pltpu.VMEM((2, local_k, fields, columns), bf16),
            pltpu.VMEM(tables.shape, bf16),
            dma((2, pieces)), dma, pltpu.SemaphoreType.REGULAR((nkx // 2,)),
            pltpu.VMEM((16 * Y, 16 * Y), bf16),
            pltpu.VMEM((columns, local_k), jnp.float32),
            pltpu.VMEM((columns // 128, fields * local_k, 128), jnp.float32),
            pltpu.VMEM((2 * fields, Y, local_m, local_k), bf16),
            pltpu.VMEM((2 * fields, own_rows, points_x, local_k), bf16),
            pltpu.VMEM((2 * fields, points_x, own_rows * local_k), bf16),
            pltpu.VMEM((2 * fields, ncz, share_x, own_rows * local_k), bf16),
            pltpu.VMEM((fields, own_rows * share_x, MZ), jnp.float32),
            pltpu.VMEM((own_rows * share_x, MZ), jnp.float32),
            pltpu.VMEM((own_rows * share_x, MZ), bf16),
            pltpu.VMEM((fields, ncz, share_x, own_rows * local_k), bf16),
            pltpu.VMEM((fields, points_x, own_rows * local_k), bf16),
            pltpu.VMEM((fields, own_rows, points_x, local_k), bf16),
            pltpu.VMEM((fields, Y, local_m, local_k), bf16),
            dma, dma((2 * fields,)), dma, dma((2 * fields,)),
            dma, dma((fields,)), dma, dma((fields,)),
        ],
        compiler_params=pltpu.CompilerParams(has_side_effects=True, vmem_limit_bytes=52 * 2**20, collective_id=0),
    )(field_modes, cotangent, tables)
    return pl.pallas_call(
        deliver,
        out_shape=jax.ShapeDtypeStruct(field_modes.shape, bf16),
        in_specs=[pl.BlockSpec(memory_space=pl.ANY)],
        out_specs=hbm,
        scratch_shapes=[dma],
        compiler_params=pltpu.CompilerParams(vmem_limit_bytes=2 * 2**20),
    )(out.reshape(columns // 128, local_k, fields, 128))


def solution(mesh):
    return jax.shard_map(
        functools.partial(on_device, mesh.shape["kx"], mesh.shape["cz"]),
        mesh=mesh,
        in_specs=(P("cz", None, "kx"), P("cz", None, "kx")),
        out_specs=P("cz", None, "kx"),
        check_vma=False,
    )
```

```python
import functools
import math

import jax
import jax.numpy as jnp
import numpy as np
from jax import lax
from jax.experimental import pallas as pl
from jax.experimental.pallas import tpu as pltpu
from jax.sharding import PartitionSpec as P

MZ = 768
Y = 16
MESH = pl.DeviceIdType.MESH


def cosine_table(rows, columns):
    position = (np.arange(columns)[None, :] * (2 * np.arange(rows)[:, None] + 1)) % (4 * rows)
    return np.cos(np.pi * position / (2 * rows)).astype(np.float32)


def hartley_table(points):
    index = np.arange(points)
    phases = 2.0 * np.pi * ((index[:, None] * index[None, :]) % points) / points
    return (np.cos(phases) + np.sin(phases)) / math.sqrt(points)


def matmul(a, b):
    return jnp.dot(a, b, preferred_element_type=jnp.float32)


def matmul_t(a, b):
    return lax.dot_general(a, b, (((1,), (1,)), ((), ())), preferred_element_type=jnp.float32)


def kernel(
    nkx, ncz, pieces,
    field_modes, cotangent, tables_in,
    out,
    raw, tables, raw_sem, table_sem, ready,
    weave, wide, stage, rows, held, mixed, parts, points, total, flux, lowered, turned, result, landed,
    in_send, in_recv, swap_send, swap_recv, back_send, back_recv, out_send, out_recv,
):
    local_k, fields, columns = field_modes.shape
    rows_y = rows.shape[1]
    local_m = columns // rows_y
    own_rows = rows_y // nkx
    points_x = local_m * nkx
    points_z = points.shape[2]
    modes_z = local_k * ncz
    share_x = points_x // ncz
    aligned = local_k % 128 == 0
    i, j = lax.axis_index("kx"), lax.axis_index("cz")
    ahead = 3
    order = ((0, 2), (1, 0), (1, 1), (1, 3), (0, 0), (0, 1), (0, 3), (1, 2))

    places = nkx // 2
    place, column = i // 2, lax.rem(i, 2)
    above, below = place + 1 < places, place > 0
    inner = jnp.logical_or(place == places // 2 - 1, place == places // 2)
    near = 1 + jnp.where(above, 1, 0) + jnp.where(below, 1, 0)

    def at(row_owner, mode_owner):
        return {"kx": row_owner, "cz": mode_owner}

    def wait(ref, sem):
        pltpu.make_async_copy(ref, ref, sem).wait()

    piece = columns // pieces
    raw_copies = [
        [
            pltpu.make_async_copy(
                array.at[:, :, pl.ds(p * piece, piece)], raw.at[a, :, :, pl.ds(p * piece, piece)], raw_sem.at[a, p]
            )
            for p in range(pieces)
        ]
        for a, array in enumerate((field_modes, cotangent))
    ]
    table_copy = pltpu.make_async_copy(tables_in, tables, table_sem)
    for copy in raw_copies[0]:
        copy.start()
    barrier = pltpu.get_barrier_semaphore()

    def signal_near(sem):
        pl.semaphore_signal(sem, inc=1, device_id=at(place * 2 + 1 - column, j), device_id_type=MESH)

        @pl.when(above)
        def _():
            pl.semaphore_signal(sem, inc=1, device_id=at(i + 2, j), device_id_type=MESH)

        @pl.when(below)
        def _():
            pl.semaphore_signal(sem, inc=1, device_id=at(i - 2, j), device_id_type=MESH)

    signal_near(barrier)
    for step in range(1, ncz):
        pl.semaphore_signal(barrier, inc=1, device_id=at(i, lax.rem(j + step, ncz)), device_id_type=MESH)

    hartley = tables.at[pl.ds(0, points_x)]
    lifts = [tables.at[pl.ds(points_x + n * modes_z, modes_z)] for n in range(2)]
    chunk, group = 128, 16
    block = group * rows_y
    row = lax.broadcasted_iota(jnp.int32, (block, block), 0)
    lane = lax.broadcasted_iota(jnp.int32, (block, block), 1)
    moved = lax.rem(row, group) * rows_y + row // group
    weave[...] = jnp.where(moved == lane, 1.0, 0.0).astype(jnp.bfloat16)

    def prepare(h, between=None):
        a, f = order[h]

        def turn(step, carry):
            here = pl.ds(pl.multiple_of(step * block, block), block)
            value = matmul_t(weave[...], raw[a, :, f, here]).astype(jnp.bfloat16)
            rows[h, :, pl.ds(pl.multiple_of(step * group, group), group), :] = value.reshape(rows_y, group, local_k)
            return carry

        if h >= 2:
            lax.fori_loop(0, columns // block, turn, 0)
        else:
            span = columns // block // pieces
            for p in range(pieces):
                raw_copies[a][p].wait()
                lax.fori_loop(p * span, (p + 1) * span, turn, 0)
                if between is not None:
                    between(p)

    def in_place(h, start=0, count=local_m):
        return held.at[h, :, pl.ds(pl.multiple_of(i * local_m, local_m) + start, count)]

    def send_in(h, target, start=0, count=local_m):
        pltpu.make_async_remote_copy(
            src_ref=rows.at[h, pl.ds(target * own_rows, own_rows), pl.ds(start, count)],
            dst_ref=in_place(h, start, count),
            send_sem=in_send,
            recv_sem=in_recv.at[h],
            device_id=at(target, j),
            device_id_type=MESH,
        ).start()

    def keep_in(h):
        pltpu.make_async_copy(rows.at[h, pl.ds(i * own_rows, own_rows)], in_place(h), in_recv.at[h]).start()

    def flip(index, step):
        bit = 1
        target = index
        while bit < nkx:
            if step & bit:
                target = target + bit * (1 - 2 * lax.rem(index // bit, 2))
            bit *= 2
        return target

    half = nkx // 2
    within = list(range(1, half))
    across = [s for p in range(half // 2, places) for s in (2 * p + 1, 2 * p)]

    def targets(chosen):
        if nkx & (nkx - 1):
            return [lax.rem(i + s, nkx) for s in chosen]
        return [flip(i, s) for s in chosen]

    def send_at_distance(h, distance, start=0, count=local_m):
        for hops, side in ((distance, 0), (distance - 1, 1)):
            facing = place * 2 + (column if side == 0 else 1 - column)
            if hops == 0:
                send_in(h, facing, start, count)
            elif hops < places:
                @pl.when(place + hops < places)
                def _():
                    send_in(h, facing + 2 * hops, start, count)

                @pl.when(place >= hops)
                def _():
                    send_in(h, facing - 2 * hops, start, count)

    part_m = local_m // pieces

    def begin(p):
        if p == 0:
            pl.semaphore_wait(barrier, near + ncz - 1)
            if places > 1:
                signal_near(ready.at[0])
        if p == pieces - 1:
            for copy in raw_copies[1]:
                copy.start()
        send_at_distance(0, 1, p * part_m, part_m)

    prepare(0, begin)
    for distance in range(2, places + 1):
        pl.semaphore_wait(ready.at[distance - 2], near)
        if distance < places:
            signal_near(ready.at[distance - 1])
        send_at_distance(0, distance)
    keep_in(0)
    table_copy.start()

    def launch(h):
        if h < 2 * fields:
            prepare(h)
            for target in targets(within + across):
                send_in(h, target)
            keep_in(h)

    for h in range(1, ahead):
        launch(h)

    def share_rows(q):
        return pl.ds(pl.multiple_of(q * share_x, share_x), share_x)

    def lanes(r):
        return slice(r * local_k, (r + 1) * local_k)

    def transform(target, source):
        if aligned:
            joined = source[0] if len(source) == 1 else jnp.concatenate(source, axis=1)
            value = matmul(hartley[...], joined).astype(jnp.bfloat16)
            for r in range(own_rows):
                target(r, value[:, lanes(r)])
        else:
            for r in range(own_rows):
                target(r, matmul(hartley[...], source[r]).astype(jnp.bfloat16))

    def mix(h):
        wait(held.at[h], in_recv.at[h])

        def keep(r, value):
            mixed[h, :, lanes(r)] = value

        transform(keep, [held[h, r] for r in range(own_rows)])
        for step in range(1, ncz):
            q = lax.rem(j + step, ncz)
            pltpu.make_async_remote_copy(
                src_ref=mixed.at[h, share_rows(q), :],
                dst_ref=parts.at[h, j],
                send_sem=swap_send,
                recv_sem=swap_recv.at[h],
                device_id=at(i, q),
                device_id_type=MESH,
            ).start()
        pltpu.make_async_copy(mixed.at[h, share_rows(j), :], parts.at[h, j], swap_recv.at[h]).start()

    block_z = 256 if points_z % 256 == 0 else points_z

    def lift(h, use):
        wait(parts.at[h], swap_recv.at[h])
        table = lifts[order[h][0]]

        def one(step, carry):
            here = pl.ds(pl.multiple_of(step * block_z, block_z), block_z)
            if aligned:
                joined = jnp.concatenate(
                    [
                        jnp.concatenate([parts[h, q, :, lanes(r)] for q in range(ncz)], axis=1)
                        for r in range(own_rows)
                    ],
                    axis=0,
                )
                use(slice(None), here, matmul(joined, table[:, here]))
            else:
                for r in range(own_rows):
                    value = matmul(parts[h, 0, :, lanes(r)], table[0:local_k, here])
                    for q in range(1, ncz):
                        value += matmul(parts[h, q, :, lanes(r)], table[q * local_k:(q + 1) * local_k, here])
                    use(slice(r * share_x, (r + 1) * share_x), here, value)
            return carry

        lax.fori_loop(0, points_z // block_z, one, 0)

    def leave(f):
        if aligned:
            value = matmul_t(flux[...], lifts[0][...]).astype(jnp.bfloat16)
            for q in range(ncz):
                for r in range(own_rows):
                    lowered[f, q, :, lanes(r)] = value[r * share_x:(r + 1) * share_x, lanes(q)]
        else:
            for q in range(ncz):
                for r in range(own_rows):
                    lowered[f, q, :, lanes(r)] = matmul_t(
                        flux[r * share_x:(r + 1) * share_x, :], lifts[0][q * local_k:(q + 1) * local_k, :]
                    ).astype(jnp.bfloat16)
        for step in range(1, ncz):
            q = lax.rem(j + step, ncz)
            pltpu.make_async_remote_copy(
                src_ref=lowered.at[f, q],
                dst_ref=turned.at[f, share_rows(j), :],
                send_sem=back_send,
                recv_sem=back_recv.at[f],
                device_id=at(i, q),
                device_id_type=MESH,
            ).start()
        pltpu.make_async_copy(lowered.at[f, j], turned.at[f, share_rows(j), :], back_recv.at[f]).start()

    def out_block(f, target):
        return result.at[f, :, pl.ds(pl.multiple_of(target * local_m, local_m), local_m)]

    def out_place(f):
        return landed.at[f, pl.ds(i * own_rows, own_rows)]

    def finish(f):
        wait(turned.at[f], back_recv.at[f])

        def keep(r, value):
            result[f, r] = value

        transform(keep, [turned[f, :, lanes(r)] for r in range(own_rows)])
        pltpu.make_async_copy(out_block(f, i), out_place(f), out_recv.at[f]).start()

    def depart(f, chosen):
        for target in targets(chosen):
            pltpu.make_async_remote_copy(
                src_ref=out_block(f, target),
                dst_ref=out_place(f),
                send_sem=out_send,
                recv_sem=out_recv.at[f],
                device_id=at(target, j),
                device_id_type=MESH,
            ).start()

    outer = jnp.logical_not(inner)

    def settle(f):
        wait(landed.at[f], out_recv.at[f])
        for y in range(rows_y):
            wide[pl.ds(y, local_m, stride=rows_y), :] = landed[f, y].astype(jnp.float32)

        def lay(step, carry):
            here = pl.ds(pl.multiple_of(step * chunk, chunk), chunk)
            stage[step, pl.ds(f, local_k, stride=fields), :] = wide[here, :].T
            if f == 2:
                out[step] = stage[step].astype(jnp.bfloat16)
            return carry

        lax.fori_loop(0, columns // chunk, lay, 0, unroll=f in (2, 3))

    def keep(h):
        def use(part, here, value):
            points[h, part, here] = value
        return use

    def keep_and_flux(h):
        def use(part, here, value):
            points[h, part, here] = value
            flux[part, here] = (value * points[0, part, here]).astype(jnp.bfloat16)
        return use

    def first(part, here, value):
        total[part, here] = points[1, part, here] * value

    def add(h):
        def use(part, here, value):
            total[part, here] += points[h, part, here] * value
        return use

    def last(part, here, value):
        flux[part, here] = (total[part, here] + 2.0 * value * points[0, part, here]).astype(jnp.bfloat16)

    table_copy.wait()
    mix(0)
    launch(ahead)
    mix(1)
    launch(ahead + 1)
    lift(0, keep(0))
    mix(2)
    launch(ahead + 2)
    lift(1, keep_and_flux(1))
    leave(0)
    mix(3)
    launch(ahead + 3)
    lift(2, keep_and_flux(2))
    leave(1)
    finish(0)
    mix(4)
    launch(ahead + 4)
    lift(3, keep_and_flux(3))
    leave(3)
    finish(1)

    @pl.when(inner)
    def _():
        depart(0, within + across)
        depart(1, within + across)

    mix(5)
    launch(ahead + 5)
    lift(4, first)
    finish(3)

    @pl.when(inner)
    def _():
        depart(3, within + across)

    mix(6)
    launch(ahead + 6)
    lift(5, add(2))
    mix(7)

    @pl.when(outer)
    def _():
        for f in (0, 1, 3):
            depart(f, within + across)

    lift(6, add(3))
    lift(7, last)
    leave(2)
    finish(2)
    depart(2, within + across)

    for f in (0, 1, 3, 2):
        settle(f)

    wait(rows.at[:, pl.ds(0, rows_y - own_rows)], in_send)
    wait(mixed.at[:, pl.ds(0, points_x - share_x), :], swap_send)
    wait(lowered.at[:, pl.ds(0, ncz - 1)], back_send)
    wait(landed.at[:, pl.ds(0, rows_y - own_rows)], out_send)


def kernel_halves(
    nkx, ncz, pieces,
    field_modes, cotangent, tables_in,
    out,
    raw, tables, raw_sem, table_sem, ready,
    weave, wide, stage, rows, held, kept, mixed, vertical, other, total, flux, lowered, result, beyond, landed, crossed,
    in_send, in_recv, out_send, out_recv, cross_recv,
):
    local_k, fields, columns = field_modes.shape
    rows_y = rows.shape[1]
    local_m = columns // rows_y
    points_x = local_m * nkx
    points_z = vertical.shape[1]
    modes_z = local_k * ncz
    members = nkx // 2
    half_m = members * local_m
    i, j = lax.axis_index("kx"), lax.axis_index("cz")
    side, member = i // members, lax.rem(i, members)
    my_row = member * ncz + j
    order = ((0, 2), (0, 0), (1, 0), (0, 1), (1, 1), (0, 3), (1, 3), (1, 2))
    shared = (True, False) * fields
    ahead = 4

    places = nkx // 2
    place, column = i // 2, lax.rem(i, 2)
    above, below = place + 1 < places, place > 0
    near = ncz + jnp.where(above, 1, 0) + jnp.where(below, 1, 0)

    def at(row_owner, mode_owner):
        return {"kx": row_owner, "cz": mode_owner}

    def wait(ref, sem):
        pltpu.make_async_copy(ref, ref, sem).wait()

    piece = columns // pieces
    raw_copies = [
        [
            pltpu.make_async_copy(
                array.at[:, :, pl.ds(p * piece, piece)], raw.at[a, :, :, pl.ds(p * piece, piece)], raw_sem.at[a, p]
            )
            for p in range(pieces)
        ]
        for a, array in enumerate((field_modes, cotangent))
    ]
    table_copy = pltpu.make_async_copy(tables_in, tables, table_sem)
    for copy in raw_copies[0]:
        copy.start()
    barrier = pltpu.get_barrier_semaphore()

    def signal_near(sem):
        pl.semaphore_signal(sem, inc=1, device_id=at(place * 2 + 1 - column, j), device_id_type=MESH)

        @pl.when(above)
        def _():
            pl.semaphore_signal(sem, inc=1, device_id=at(i + 2, j), device_id_type=MESH)

        @pl.when(below)
        def _():
            pl.semaphore_signal(sem, inc=1, device_id=at(i - 2, j), device_id_type=MESH)

        for step in range(1, ncz):
            pl.semaphore_signal(sem, inc=1, device_id=at(i, lax.rem(j + step, ncz)), device_id_type=MESH)

    signal_near(barrier)
    hartley = tables.at[pl.ds(0, points_x)]
    lifts = [tables.at[pl.ds(points_x + n * modes_z, modes_z)] for n in range(2)]
    chunk, group = 128, 16
    block = group * rows_y
    row = lax.broadcasted_iota(jnp.int32, (block, block), 0)
    lane = lax.broadcasted_iota(jnp.int32, (block, block), 1)
    moved = lax.rem(row, group) * rows_y + row // group
    weave[...] = jnp.where(moved == lane, 1.0, 0.0).astype(jnp.bfloat16)

    def prepare(h, between=None):
        a, f = order[h]

        def turn(step, carry):
            here = pl.ds(pl.multiple_of(step * block, block), block)
            value = matmul_t(weave[...], raw[a, :, f, here]).astype(jnp.bfloat16)
            rows[h, :, pl.ds(pl.multiple_of(step * group, group), group), :] = value.reshape(rows_y, group, local_k)
            return carry

        if all(order[n][0] != a for n in range(h)):
            span = columns // block // pieces
            for p in range(pieces):
                raw_copies[a][p].wait()
                lax.fori_loop(p * span, (p + 1) * span, turn, 0)
                if between is not None:
                    between(p)
        else:
            lax.fori_loop(0, columns // block, turn, 0)

    my_lanes = pl.ds(pl.multiple_of(j * local_k, local_k), local_k)

    def in_place(h, start=0, count=local_m):
        if shared[h]:
            return held.at[h // 2, pl.ds(pl.multiple_of(i * local_m, local_m) + start, count), my_lanes]
        return kept.at[h // 2, pl.ds(pl.multiple_of(member * local_m, local_m) + start, count), my_lanes]

    def send_in(h, row_owner, mode_owner, start=0, count=local_m):
        pltpu.make_async_remote_copy(
            src_ref=rows.at[h, lax.rem(row_owner, members) * ncz + mode_owner, pl.ds(start, count)],
            dst_ref=in_place(h, start, count),
            send_sem=in_send,
            recv_sem=in_recv.at[h],
            device_id=at(row_owner, mode_owner),
            device_id_type=MESH,
        ).start()

    def keep_in(h):
        pltpu.make_async_copy(rows.at[h, my_row], in_place(h), in_recv.at[h]).start()

    def flip(index, step):
        bit = 1
        target = index
        while bit < nkx:
            if step & bit:
                target = target + bit * (1 - 2 * lax.rem(index // bit, 2))
            bit *= 2
        return target

    within = list(range(1, members))
    across = [s for p in range(members // 2, places) for s in (2 * p + 1, 2 * p)]

    def to_all(steps, send):
        for s in steps:
            target = flip(i, s)

            def one(step, carry):
                send(target, lax.rem(j + step, ncz))
                return carry

            lax.fori_loop(0 if s else 1, ncz, one, 0)

    def hop_away(hops, side_step, use):
        facing = place * 2 + (1 - column if side_step else column)
        if hops == 0:
            use(facing)
        elif hops < places:
            @pl.when(place + hops < places)
            def _():
                use(facing + 2 * hops)

            @pl.when(place >= hops)
            def _():
                use(facing - 2 * hops)

    def each_other(send, target):
        def one(step, carry):
            send(target, lax.rem(j + step, ncz))
            return carry

        lax.fori_loop(1, ncz, one, 0)

    part_m = local_m // pieces

    def begin(p):
        if p == 0:
            pl.semaphore_wait(barrier, near)
            signal_near(ready.at[0])
        if p == pieces - 1:
            for copy in raw_copies[1]:
                copy.start()
        hop_away(1, False, lambda t: send_in(0, t, j, p * part_m, part_m))
        hop_away(0, True, lambda t: send_in(0, t, j, p * part_m, part_m))

    prepare(0, begin)
    send_0 = functools.partial(send_in, 0)
    each_other(send_0, i)
    for distance in range(2, places + 2):
        pl.semaphore_wait(ready.at[distance - 2], near)
        if distance < places + 1:
            signal_near(ready.at[distance - 1])
        if distance <= places:
            hop_away(distance, False, lambda t: send_in(0, t, j))
            hop_away(distance - 1, True, lambda t: send_in(0, t, j))
        hop_away(distance - 1, False, lambda t: each_other(send_0, t))
        hop_away(distance - 2, True, lambda t: each_other(send_0, t))
    keep_in(0)
    table_copy.start()

    def launch(h):
        if h < 2 * fields:
            prepare(h)
            to_all([0] + within + (across if shared[h] else []), functools.partial(send_in, h))
            keep_in(h)

    for h in range(1, ahead):
        launch(h)

    half_lanes = modes_z // 2
    parts = [slice(n * half_lanes, (n + 1) * half_lanes) for n in range(2)]
    block_z = 256 if points_z % 256 == 0 else points_z

    def own_m(which):
        return pl.ds(pl.multiple_of(which * half_m, half_m), half_m)

    def gather(h, use):
        source = held.at[h // 2] if shared[h] else kept.at[h // 2]
        wait(source, in_recv.at[h])
        for part in parts:
            table = hartley[...] if shared[h] else hartley[:, own_m(side)]
            mixed[:, part] = matmul(table, source[:, part]).astype(jnp.bfloat16)
        launch(h + ahead)
        lift_table = lifts[order[h][0]]

        def one(step, carry):
            here = pl.ds(pl.multiple_of(step * block_z, block_z), block_z)
            use(here, matmul(mixed[...], lift_table[:, here]))
            return carry

        lax.fori_loop(0, points_z // block_z, one, 0)

    def lower():
        for part in parts:
            lowered[:, part] = matmul_t(flux[...], lifts[0][part, :]).astype(jnp.bfloat16)

    def out_block(ref, row_owner, mode_owner):
        first_m = pl.multiple_of(lax.rem(row_owner, members) * local_m, local_m)
        return ref.at[pl.ds(first_m, local_m), pl.ds(pl.multiple_of(mode_owner * local_k, local_k), local_k)]

    def send_out(source, target, sem, row_owner, mode_owner):
        pltpu.make_async_remote_copy(
            src_ref=out_block(source, row_owner, mode_owner),
            dst_ref=target,
            send_sem=out_send,
            recv_sem=sem,
            device_id=at(row_owner, mode_owner),
            device_id_type=MESH,
        ).start()

    def finish(f):
        lower()
        if f == 2:
            for part in parts:
                beyond[:, part] = matmul(hartley[own_m(1 - side), :], lowered[:, part]).astype(jnp.bfloat16)
            to_all(across, functools.partial(send_out, beyond, crossed.at[my_row], cross_recv))
        for part in parts:
            result[f, :, part] = matmul(hartley[own_m(side), :], lowered[:, part]).astype(jnp.bfloat16)
        pltpu.make_async_copy(out_block(result.at[f], i, j), landed.at[f, my_row], out_recv.at[f]).start()
        to_all([0] + within, functools.partial(send_out, result.at[f], landed.at[f, my_row], out_recv.at[f]))

    def keep(target):
        def use(here, value):
            target[:, here] = value
        return use

    def multiply(first):
        def use(here, value):
            flux[:, here] = (value * vertical[:, here]).astype(jnp.bfloat16)
            product = value * other[:, here]
            total[:, here] = product if first else total[:, here] + product
        return use

    def last(here, value):
        flux[:, here] = (total[:, here] + 2.0 * value * vertical[:, here]).astype(jnp.bfloat16)

    table_copy.wait()
    gather(0, keep(vertical))
    for h, f in ((1, 0), (3, 1), (5, 3)):
        gather(h, keep(other))
        gather(h + 1, multiply(h == 1))
        finish(f)
    gather(7, last)
    finish(2)

    def settle(f):
        wait(landed.at[f], out_recv.at[f])
        if f == 2:
            wait(crossed, cross_recv)
        for y in range(rows_y):
            value = landed[f, y].astype(jnp.float32)
            if f == 2:
                value += crossed[y].astype(jnp.float32)
            wide[pl.ds(y, local_m, stride=rows_y), :] = value

        def lay(step, carry):
            here = pl.ds(pl.multiple_of(step * chunk, chunk), chunk)
            stage[step, pl.ds(f, local_k, stride=fields), :] = wide[here, :].T
            if f == 2:
                out[step] = stage[step].astype(jnp.bfloat16)
            return carry

        lax.fori_loop(0, columns // chunk, lay, 0, unroll=f == 2)

    for f in (0, 1, 3, 2):
        settle(f)

    wait(rows.at[pl.ds(0, fields)], in_send)
    wait(rows.at[:, pl.ds(0, rows_y - 1)], in_send)
    wait(landed.at[:, pl.ds(0, rows_y - 1)], out_send)
    wait(crossed, out_send)


def deliver(tiles, out, sem):
    for n in range(tiles.shape[0]):
        pltpu.make_async_copy(tiles.at[n], out.at[:, :, pl.ds(n * 128, 128)], sem).start()
    pltpu.make_async_copy(out, out, sem).wait()


def on_device(nkx, ncz, field_modes, cotangent):
    local_k, fields, columns = field_modes.shape
    local_m = columns // Y
    modes_z, points_x = local_k * ncz, local_m * nkx
    own_rows = Y // nkx
    share_x = points_x // ncz
    bf16 = jnp.bfloat16
    pieces = next(p for p in (3, 2, 1) if columns % (p * 16 * Y) == 0 or p == 1)

    cosines = cosine_table(MZ, modes_z)
    synthesis = (cosines * math.sqrt(2.0 / modes_z)).astype(bf16).T
    projection = (cosines * math.sqrt(2.0 / MZ)).astype(bf16).T
    hartley = hartley_table(points_x).astype(np.float32).astype(bf16)
    tables = jnp.asarray(np.concatenate([hartley, synthesis, projection], axis=0))

    hbm = pl.BlockSpec(memory_space=pltpu.HBM)
    dma = pltpu.SemaphoreType.DMA
    whole_rows = nkx // 2 * ncz == Y and nkx & (nkx - 1) == 0 and local_k % 128 == 0
    if whole_rows:
        members = nkx // 2
        body = kernel_halves
        scratch = [
            pltpu.VMEM((fields, points_x, modes_z), bf16),
            pltpu.VMEM((fields, members * local_m, modes_z), bf16),
            pltpu.VMEM((points_x, modes_z), bf16),
            pltpu.VMEM((points_x, MZ), jnp.float32),
            pltpu.VMEM((points_x, MZ), jnp.float32),
            pltpu.VMEM((points_x, MZ), jnp.float32),
            pltpu.VMEM((points_x, MZ), bf16),
            pltpu.VMEM((points_x, modes_z), bf16),
            pltpu.VMEM((fields, members * local_m, modes_z), bf16),
            pltpu.VMEM((members * local_m, modes_z), bf16),
            pltpu.VMEM((fields, Y, local_m, local_k), bf16),
            pltpu.VMEM((Y, local_m, local_k), bf16),
            dma, dma((2 * fields,)), dma, dma((fields,)), dma,
        ]
    else:
        body = kernel
        scratch = [
            pltpu.VMEM((2 * fields, own_rows, points_x, local_k), bf16),
            pltpu.VMEM((2 * fields, points_x, own_rows * local_k), bf16),
            pltpu.VMEM((2 * fields, ncz, share_x, own_rows * local_k), bf16),
            pltpu.VMEM((fields, own_rows * share_x, MZ), jnp.float32),
            pltpu.VMEM((own_rows * share_x, MZ), jnp.float32),
            pltpu.VMEM((own_rows * share_x, MZ), bf16),
            pltpu.VMEM((fields, ncz, share_x, own_rows * local_k), bf16),
            pltpu.VMEM((fields, points_x, own_rows * local_k), bf16),
            pltpu.VMEM((fields, own_rows, points_x, local_k), bf16),
            pltpu.VMEM((fields, Y, local_m, local_k), bf16),
            dma, dma((2 * fields,)), dma, dma((2 * fields,)),
            dma, dma((fields,)), dma, dma((fields,)),
        ]
    out = pl.pallas_call(
        functools.partial(body, nkx, ncz, pieces),
        out_shape=jax.ShapeDtypeStruct((columns // 128, fields * local_k, 128), bf16),
        in_specs=[hbm] * 3,
        out_specs=pl.BlockSpec(memory_space=pltpu.VMEM),
        scratch_shapes=[
            pltpu.VMEM((2, local_k, fields, columns), bf16),
            pltpu.VMEM(tables.shape, bf16),
            dma((2, pieces)), dma, pltpu.SemaphoreType.REGULAR((nkx // 2 + 1,)),
            pltpu.VMEM((16 * Y, 16 * Y), bf16),
            pltpu.VMEM((columns, local_k), jnp.float32),
            pltpu.VMEM((columns // 128, fields * local_k, 128), jnp.float32),
            pltpu.VMEM((2 * fields, Y, local_m, local_k), bf16),
            *scratch,
        ],
        compiler_params=pltpu.CompilerParams(has_side_effects=True, vmem_limit_bytes=52 * 2**20, collective_id=0),
    )(field_modes, cotangent, tables)
    return pl.pallas_call(
        deliver,
        out_shape=jax.ShapeDtypeStruct(field_modes.shape, bf16),
        in_specs=[pl.BlockSpec(memory_space=pl.ANY)],
        out_specs=hbm,
        scratch_shapes=[dma],
        compiler_params=pltpu.CompilerParams(vmem_limit_bytes=2 * 2**20),
    )(out.reshape(columns // 128, local_k, fields, 128))


def solution(mesh):
    return jax.shard_map(
        functools.partial(on_device, mesh.shape["kx"], mesh.shape["cz"]),
        mesh=mesh,
        in_specs=(P("cz", None, "kx"), P("cz", None, "kx")),
        out_specs=P("cz", None, "kx"),
        check_vma=False,
    )
```

```python
import functools
import math

import jax
import jax.numpy as jnp
import numpy as np
from jax import lax
from jax.experimental import pallas as pl
from jax.experimental.pallas import tpu as pltpu
from jax.sharding import PartitionSpec as P

MZ = 768
Y = 16
MESH = pl.DeviceIdType.MESH


def cosine_table(rows, columns):
    position = (np.arange(columns)[None, :] * (2 * np.arange(rows)[:, None] + 1)) % (4 * rows)
    return np.cos(np.pi * position / (2 * rows)).astype(np.float32)


def hartley_table(points):
    index = np.arange(points)
    phases = 2.0 * np.pi * ((index[:, None] * index[None, :]) % points) / points
    return (np.cos(phases) + np.sin(phases)) / math.sqrt(points)


def matmul(a, b):
    return jnp.dot(a, b, preferred_element_type=jnp.float32)


def matmul_t(a, b):
    return lax.dot_general(a, b, (((1,), (1,)), ((), ())), preferred_element_type=jnp.float32)


def kernel(
    nkx, ncz, pieces,
    field_modes, cotangent, tables_in,
    out,
    raw, tables, raw_sem, table_sem, ready,
    weave, wide, stage, rows, held, mixed, parts, points, total, flux, lowered, turned, result, landed,
    in_send, in_recv, swap_send, swap_recv, back_send, back_recv, out_send, out_recv,
):
    local_k, fields, columns = field_modes.shape
    rows_y = rows.shape[1]
    local_m = columns // rows_y
    own_rows = rows_y // nkx
    points_x = local_m * nkx
    points_z = points.shape[2]
    modes_z = local_k * ncz
    share_x = points_x // ncz
    aligned = local_k % 128 == 0
    i, j = lax.axis_index("kx"), lax.axis_index("cz")
    ahead = 3
    order = ((0, 2), (1, 0), (1, 1), (1, 3), (0, 0), (0, 1), (0, 3), (1, 2))

    places = nkx // 2
    place, column = i // 2, lax.rem(i, 2)
    above, below = place + 1 < places, place > 0
    inner = jnp.logical_or(place == places // 2 - 1, place == places // 2)
    near = 1 + jnp.where(above, 1, 0) + jnp.where(below, 1, 0)

    def at(row_owner, mode_owner):
        return {"kx": row_owner, "cz": mode_owner}

    def wait(ref, sem):
        pltpu.make_async_copy(ref, ref, sem).wait()

    piece = columns // pieces
    raw_copies = [
        [
            pltpu.make_async_copy(
                array.at[:, :, pl.ds(p * piece, piece)], raw.at[a, :, :, pl.ds(p * piece, piece)], raw_sem.at[a, p]
            )
            for p in range(pieces)
        ]
        for a, array in enumerate((field_modes, cotangent))
    ]
    table_copy = pltpu.make_async_copy(tables_in, tables, table_sem)
    for copy in raw_copies[0]:
        copy.start()
    barrier = pltpu.get_barrier_semaphore()

    def signal_near(sem):
        pl.semaphore_signal(sem, inc=1, device_id=at(place * 2 + 1 - column, j), device_id_type=MESH)

        @pl.when(above)
        def _():
            pl.semaphore_signal(sem, inc=1, device_id=at(i + 2, j), device_id_type=MESH)

        @pl.when(below)
        def _():
            pl.semaphore_signal(sem, inc=1, device_id=at(i - 2, j), device_id_type=MESH)

    signal_near(barrier)
    for step in range(1, ncz):
        pl.semaphore_signal(barrier, inc=1, device_id=at(i, lax.rem(j + step, ncz)), device_id_type=MESH)

    hartley = tables.at[pl.ds(0, points_x)]
    lifts = [tables.at[pl.ds(points_x + n * modes_z, modes_z)] for n in range(2)]
    chunk, group = 128, 16
    block = group * rows_y
    row = lax.broadcasted_iota(jnp.int32, (block, block), 0)
    lane = lax.broadcasted_iota(jnp.int32, (block, block), 1)
    moved = lax.rem(row, group) * rows_y + row // group
    weave[...] = jnp.where(moved == lane, 1.0, 0.0).astype(jnp.bfloat16)

    def prepare(h, between=None):
        a, f = order[h]

        def turn(step, carry):
            here = pl.ds(pl.multiple_of(step * block, block), block)
            value = matmul_t(weave[...], raw[a, :, f, here]).astype(jnp.bfloat16)
            rows[h, :, pl.ds(pl.multiple_of(step * group, group), group), :] = value.reshape(rows_y, group, local_k)
            return carry

        if h >= 2:
            lax.fori_loop(0, columns // block, turn, 0)
        else:
            span = columns // block // pieces
            for p in range(pieces):
                raw_copies[a][p].wait()
                lax.fori_loop(p * span, (p + 1) * span, turn, 0)
                if between is not None:
                    between(p)

    def in_place(h, start=0, count=local_m):
        return held.at[h, :, pl.ds(pl.multiple_of(i * local_m, local_m) + start, count)]

    def send_in(h, target, start=0, count=local_m):
        pltpu.make_async_remote_copy(
            src_ref=rows.at[h, pl.ds(target * own_rows, own_rows), pl.ds(start, count)],
            dst_ref=in_place(h, start, count),
            send_sem=in_send,
            recv_sem=in_recv.at[h],
            device_id=at(target, j),
            device_id_type=MESH,
        ).start()

    def keep_in(h):
        pltpu.make_async_copy(rows.at[h, pl.ds(i * own_rows, own_rows)], in_place(h), in_recv.at[h]).start()

    def flip(index, step):
        bit = 1
        target = index
        while bit < nkx:
            if step & bit:
                target = target + bit * (1 - 2 * lax.rem(index // bit, 2))
            bit *= 2
        return target

    half = nkx // 2
    within = list(range(1, half))
    across = [s for p in range(half // 2, places) for s in (2 * p + 1, 2 * p)]

    def targets(chosen):
        if nkx & (nkx - 1):
            return [lax.rem(i + s, nkx) for s in chosen]
        return [flip(i, s) for s in chosen]

    def send_at_distance(h, distance, start=0, count=local_m):
        for hops, side in ((distance, 0), (distance - 1, 1)):
            facing = place * 2 + (column if side == 0 else 1 - column)
            if hops == 0:
                send_in(h, facing, start, count)
            elif hops < places:
                @pl.when(place + hops < places)
                def _():
                    send_in(h, facing + 2 * hops, start, count)

                @pl.when(place >= hops)
                def _():
                    send_in(h, facing - 2 * hops, start, count)

    part_m = local_m // pieces

    def begin(p):
        if p == 0:
            pl.semaphore_wait(barrier, near + ncz - 1)
            if places > 1:
                signal_near(ready.at[0])
        if p == pieces - 1:
            for copy in raw_copies[1]:
                copy.start()
        send_at_distance(0, 1, p * part_m, part_m)

    prepare(0, begin)
    for distance in range(2, places + 1):
        pl.semaphore_wait(ready.at[distance - 2], near)
        if distance < places:
            signal_near(ready.at[distance - 1])
        send_at_distance(0, distance)
    keep_in(0)
    table_copy.start()

    def launch(h):
        if h < 2 * fields:
            prepare(h)
            for target in targets(within + across):
                send_in(h, target)
            keep_in(h)

    for h in range(1, ahead):
        launch(h)

    def share_rows(q):
        return pl.ds(pl.multiple_of(q * share_x, share_x), share_x)

    def lanes(r):
        return slice(r * local_k, (r + 1) * local_k)

    def transform(target, source):
        if aligned:
            joined = source[0] if len(source) == 1 else jnp.concatenate(source, axis=1)
            value = matmul(hartley[...], joined).astype(jnp.bfloat16)
            for r in range(own_rows):
                target(r, value[:, lanes(r)])
        else:
            for r in range(own_rows):
                target(r, matmul(hartley[...], source[r]).astype(jnp.bfloat16))

    def mix(h):
        wait(held.at[h], in_recv.at[h])

        def keep(r, value):
            mixed[h, :, lanes(r)] = value

        transform(keep, [held[h, r] for r in range(own_rows)])
        for step in range(1, ncz):
            q = lax.rem(j + step, ncz)
            pltpu.make_async_remote_copy(
                src_ref=mixed.at[h, share_rows(q), :],
                dst_ref=parts.at[h, j],
                send_sem=swap_send,
                recv_sem=swap_recv.at[h],
                device_id=at(i, q),
                device_id_type=MESH,
            ).start()
        pltpu.make_async_copy(mixed.at[h, share_rows(j), :], parts.at[h, j], swap_recv.at[h]).start()

    block_z = 256 if points_z % 256 == 0 else points_z

    def lift(h, use):
        wait(parts.at[h], swap_recv.at[h])
        table = lifts[order[h][0]]

        def one(step, carry):
            here = pl.ds(pl.multiple_of(step * block_z, block_z), block_z)
            if aligned:
                joined = jnp.concatenate(
                    [
                        jnp.concatenate([parts[h, q, :, lanes(r)] for q in range(ncz)], axis=1)
                        for r in range(own_rows)
                    ],
                    axis=0,
                )
                use(slice(None), here, matmul(joined, table[:, here]))
            else:
                for r in range(own_rows):
                    value = matmul(parts[h, 0, :, lanes(r)], table[0:local_k, here])
                    for q in range(1, ncz):
                        value += matmul(parts[h, q, :, lanes(r)], table[q * local_k:(q + 1) * local_k, here])
                    use(slice(r * share_x, (r + 1) * share_x), here, value)
            return carry

        lax.fori_loop(0, points_z // block_z, one, 0)

    def leave(f):
        if aligned:
            value = matmul_t(flux[...], lifts[0][...]).astype(jnp.bfloat16)
            for q in range(ncz):
                for r in range(own_rows):
                    lowered[f, q, :, lanes(r)] = value[r * share_x:(r + 1) * share_x, lanes(q)]
        else:
            for q in range(ncz):
                for r in range(own_rows):
                    lowered[f, q, :, lanes(r)] = matmul_t(
                        flux[r * share_x:(r + 1) * share_x, :], lifts[0][q * local_k:(q + 1) * local_k, :]
                    ).astype(jnp.bfloat16)
        for step in range(1, ncz):
            q = lax.rem(j + step, ncz)
            pltpu.make_async_remote_copy(
                src_ref=lowered.at[f, q],
                dst_ref=turned.at[f, share_rows(j), :],
                send_sem=back_send,
                recv_sem=back_recv.at[f],
                device_id=at(i, q),
                device_id_type=MESH,
            ).start()
        pltpu.make_async_copy(lowered.at[f, j], turned.at[f, share_rows(j), :], back_recv.at[f]).start()

    def out_block(f, target):
        return result.at[f, :, pl.ds(pl.multiple_of(target * local_m, local_m), local_m)]

    def out_place(f):
        return landed.at[f, pl.ds(i * own_rows, own_rows)]

    def finish(f):
        wait(turned.at[f], back_recv.at[f])

        def keep(r, value):
            result[f, r] = value

        transform(keep, [turned[f, :, lanes(r)] for r in range(own_rows)])
        pltpu.make_async_copy(out_block(f, i), out_place(f), out_recv.at[f]).start()

    def depart(f, chosen):
        for target in targets(chosen):
            pltpu.make_async_remote_copy(
                src_ref=out_block(f, target),
                dst_ref=out_place(f),
                send_sem=out_send,
                recv_sem=out_recv.at[f],
                device_id=at(target, j),
                device_id_type=MESH,
            ).start()

    outer = jnp.logical_not(inner)

    def settle(f):
        wait(landed.at[f], out_recv.at[f])
        for y in range(rows_y):
            wide[pl.ds(y, local_m, stride=rows_y), :] = landed[f, y].astype(jnp.float32)

        def lay(step, carry):
            here = pl.ds(pl.multiple_of(step * chunk, chunk), chunk)
            stage[step, pl.ds(f, local_k, stride=fields), :] = wide[here, :].T
            if f == 2:
                out[step] = stage[step].astype(jnp.bfloat16)
            return carry

        lax.fori_loop(0, columns // chunk, lay, 0, unroll=f in (2, 3))

    def keep(h):
        def use(part, here, value):
            points[h, part, here] = value
        return use

    def keep_and_flux(h):
        def use(part, here, value):
            points[h, part, here] = value
            flux[part, here] = (value * points[0, part, here]).astype(jnp.bfloat16)
        return use

    def first(part, here, value):
        total[part, here] = points[1, part, here] * value

    def add(h):
        def use(part, here, value):
            total[part, here] += points[h, part, here] * value
        return use

    def last(part, here, value):
        flux[part, here] = (total[part, here] + 2.0 * value * points[0, part, here]).astype(jnp.bfloat16)

    table_copy.wait()
    mix(0)
    launch(ahead)
    mix(1)
    launch(ahead + 1)
    lift(0, keep(0))
    mix(2)
    launch(ahead + 2)
    lift(1, keep_and_flux(1))
    leave(0)
    mix(3)
    launch(ahead + 3)
    lift(2, keep_and_flux(2))
    leave(1)
    finish(0)
    mix(4)
    launch(ahead + 4)
    lift(3, keep_and_flux(3))
    leave(3)
    finish(1)

    @pl.when(inner)
    def _():
        depart(0, within + across)
        depart(1, within + across)

    mix(5)
    launch(ahead + 5)
    lift(4, first)
    finish(3)

    @pl.when(inner)
    def _():
        depart(3, within + across)

    mix(6)
    launch(ahead + 6)
    lift(5, add(2))
    mix(7)

    @pl.when(outer)
    def _():
        for f in (0, 1, 3):
            depart(f, within + across)

    lift(6, add(3))
    lift(7, last)
    leave(2)
    finish(2)
    depart(2, within + across)

    for f in (0, 1, 3, 2):
        settle(f)

    wait(rows.at[:, pl.ds(0, rows_y - own_rows)], in_send)
    wait(mixed.at[:, pl.ds(0, points_x - share_x), :], swap_send)
    wait(lowered.at[:, pl.ds(0, ncz - 1)], back_send)
    wait(landed.at[:, pl.ds(0, rows_y - own_rows)], out_send)


def kernel_halves(
    nkx, ncz, pieces,
    field_modes, cotangent, tables_in,
    out,
    raw, tables, raw_sem, table_sem, ready,
    weave, wide, stage, rows, held, kept, mixed, vertical, other, total, flux, summed, lowered, result, beyond, landed, crossed,
    in_send, in_recv, out_send, out_recv, cross_recv,
):
    local_k, fields, columns = field_modes.shape
    rows_y = rows.shape[1]
    local_m = columns // rows_y
    points_x = local_m * nkx
    points_z = vertical.shape[1]
    modes_z = local_k * ncz
    members = nkx // 2
    half_m = members * local_m
    i, j = lax.axis_index("kx"), lax.axis_index("cz")
    side, member = i // members, lax.rem(i, members)
    my_row = member * ncz + j
    order = ((0, 2), (0, 0), (1, 0), (0, 1), (1, 1), (0, 3), (1, 2), (1, 3))
    shared = (True, False, True, False, True, False, False, True)
    place_of = [sum(shared[:h]) if shared[h] else h - sum(shared[:h]) for h in range(2 * fields)]
    ahead = 6

    places = nkx // 2
    place, column = i // 2, lax.rem(i, 2)
    above, below = place + 1 < places, place > 0
    near = ncz + jnp.where(above, 1, 0) + jnp.where(below, 1, 0)

    def at(row_owner, mode_owner):
        return {"kx": row_owner, "cz": mode_owner}

    def wait(ref, sem):
        pltpu.make_async_copy(ref, ref, sem).wait()

    piece = columns // pieces
    raw_copies = [
        [
            pltpu.make_async_copy(
                array.at[:, :, pl.ds(p * piece, piece)], raw.at[a, :, :, pl.ds(p * piece, piece)], raw_sem.at[a, p]
            )
            for p in range(pieces)
        ]
        for a, array in enumerate((field_modes, cotangent))
    ]
    table_copy = pltpu.make_async_copy(tables_in, tables, table_sem)
    for copy in raw_copies[0]:
        copy.start()
    barrier = pltpu.get_barrier_semaphore()

    def signal_near(sem):
        pl.semaphore_signal(sem, inc=1, device_id=at(place * 2 + 1 - column, j), device_id_type=MESH)

        @pl.when(above)
        def _():
            pl.semaphore_signal(sem, inc=1, device_id=at(i + 2, j), device_id_type=MESH)

        @pl.when(below)
        def _():
            pl.semaphore_signal(sem, inc=1, device_id=at(i - 2, j), device_id_type=MESH)

        for step in range(1, ncz):
            pl.semaphore_signal(sem, inc=1, device_id=at(i, lax.rem(j + step, ncz)), device_id_type=MESH)

    signal_near(barrier)
    hartley = tables.at[pl.ds(0, points_x)]
    lifts = [tables.at[pl.ds(points_x + n * modes_z, modes_z)] for n in range(2)]
    chunk, group = 128, 16
    block = group * rows_y
    row = lax.broadcasted_iota(jnp.int32, (block, block), 0)
    lane = lax.broadcasted_iota(jnp.int32, (block, block), 1)
    moved = lax.rem(row, group) * rows_y + row // group
    weave[...] = jnp.where(moved == lane, 1.0, 0.0).astype(jnp.bfloat16)

    def prepare(h, between=None):
        a, f = order[h]

        def turn(step, carry):
            here = pl.ds(pl.multiple_of(step * block, block), block)
            value = matmul_t(weave[...], raw[a, :, f, here]).astype(jnp.bfloat16)
            rows[h, :, pl.ds(pl.multiple_of(step * group, group), group), :] = value.reshape(rows_y, group, local_k)
            return carry

        if all(order[n][0] != a for n in range(h)):
            span = columns // block // pieces
            for p in range(pieces):
                raw_copies[a][p].wait()
                lax.fori_loop(p * span, (p + 1) * span, turn, 0)
                if between is not None:
                    between(p)
        else:
            lax.fori_loop(0, columns // block, turn, 0)

    my_lanes = pl.ds(pl.multiple_of(j * local_k, local_k), local_k)

    def in_place(h, start=0, count=local_m):
        if shared[h]:
            return held.at[place_of[h], pl.ds(pl.multiple_of(i * local_m, local_m) + start, count), my_lanes]
        return kept.at[place_of[h], pl.ds(pl.multiple_of(member * local_m, local_m) + start, count), my_lanes]

    def send_in(h, row_owner, mode_owner, start=0, count=local_m):
        pltpu.make_async_remote_copy(
            src_ref=rows.at[h, lax.rem(row_owner, members) * ncz + mode_owner, pl.ds(start, count)],
            dst_ref=in_place(h, start, count),
            send_sem=in_send,
            recv_sem=in_recv.at[h],
            device_id=at(row_owner, mode_owner),
            device_id_type=MESH,
        ).start()

    def keep_in(h):
        pltpu.make_async_copy(rows.at[h, my_row], in_place(h), in_recv.at[h]).start()

    def flip(index, step):
        bit = 1
        target = index
        while bit < nkx:
            if step & bit:
                target = target + bit * (1 - 2 * lax.rem(index // bit, 2))
            bit *= 2
        return target

    within = list(range(1, members))
    across = [s for p in range(members // 2, places) for s in (2 * p + 1, 2 * p)]

    def to_all(steps, send):
        def one(step, carry):
            for s in steps:
                if s:
                    send(flip(i, s), lax.rem(j + step, ncz))
                else:
                    @pl.when(step > 0)
                    def _():
                        send(i, lax.rem(j + step, ncz))
            return carry

        lax.fori_loop(0, ncz, one, 0)

    def hop_away(hops, side_step, use):
        facing = place * 2 + (1 - column if side_step else column)
        if hops == 0:
            use(facing)
        elif hops < places:
            @pl.when(place + hops < places)
            def _():
                use(facing + 2 * hops)

            @pl.when(place >= hops)
            def _():
                use(facing - 2 * hops)

    def each_other(send, target):
        def one(step, carry):
            send(target, lax.rem(j + step, ncz))
            return carry

        lax.fori_loop(1, ncz, one, 0)

    part_m = local_m // pieces

    def begin(p):
        if p == 0:
            pl.semaphore_wait(barrier, near)
            signal_near(ready.at[0])
        if p == pieces - 1:
            for copy in raw_copies[1]:
                copy.start()
        hop_away(1, False, lambda t: send_in(0, t, j, p * part_m, part_m))
        hop_away(0, True, lambda t: send_in(0, t, j, p * part_m, part_m))

    prepare(0, begin)
    send_0 = functools.partial(send_in, 0)
    each_other(send_0, i)
    for distance in range(2, places + 2):
        pl.semaphore_wait(ready.at[distance - 2], near)
        if distance < places + 1:
            signal_near(ready.at[distance - 1])
        if distance <= places:
            hop_away(distance, False, lambda t: send_in(0, t, j))
            hop_away(distance - 1, True, lambda t: send_in(0, t, j))
        hop_away(distance - 1, False, lambda t: each_other(send_0, t))
        hop_away(distance - 2, True, lambda t: each_other(send_0, t))
    keep_in(0)
    table_copy.start()

    def launch(h):
        if h < 2 * fields:
            prepare(h)
            to_all([0] + within + (across if shared[h] else []), functools.partial(send_in, h))
            keep_in(h)

    for h in range(1, ahead):
        launch(h)

    half_lanes = modes_z // 2
    parts = [slice(n * half_lanes, (n + 1) * half_lanes) for n in range(2)]
    block_z = 256 if points_z % 256 == 0 else points_z

    def own_m(which):
        return pl.ds(pl.multiple_of(which * half_m, half_m), half_m)

    def gather(h, use):
        source = held.at[place_of[h]] if shared[h] else kept.at[place_of[h]]
        wait(source, in_recv.at[h])
        for part in parts:
            table = hartley[...] if shared[h] else hartley[:, own_m(side)]
            mixed[:, part] = matmul(table, source[:, part]).astype(jnp.bfloat16)
        launch(h + ahead)
        lift_table = lifts[order[h][0]]

        def one(step, carry):
            here = pl.ds(pl.multiple_of(step * block_z, block_z), block_z)
            use(here, matmul(mixed[...], lift_table[:, here]))
            return carry

        lax.fori_loop(0, points_z // block_z, one, 0)

    def lower(source):
        for part in parts:
            lowered[:, part] = matmul_t(source[...], lifts[0][part, :]).astype(jnp.bfloat16)

    def out_block(ref, row_owner, mode_owner):
        first_m = pl.multiple_of(lax.rem(row_owner, members) * local_m, local_m)
        return ref.at[pl.ds(first_m, local_m), pl.ds(pl.multiple_of(mode_owner * local_k, local_k), local_k)]

    def send_out(source, target, sem, row_owner, mode_owner):
        pltpu.make_async_remote_copy(
            src_ref=out_block(source, row_owner, mode_owner),
            dst_ref=target,
            send_sem=out_send,
            recv_sem=sem,
            device_id=at(row_owner, mode_owner),
            device_id_type=MESH,
        ).start()

    def finish(f):
        lower(summed if f == 2 else flux)
        if f == 2:
            for part in parts:
                beyond[:, part] = matmul(hartley[own_m(1 - side), :], lowered[:, part]).astype(jnp.bfloat16)
            to_all(across, functools.partial(send_out, beyond, crossed.at[my_row], cross_recv))
        for part in parts:
            result[f, :, part] = matmul(hartley[own_m(side), :], lowered[:, part]).astype(jnp.bfloat16)
        pltpu.make_async_copy(out_block(result.at[f], i, j), landed.at[f, my_row], out_recv.at[f]).start()
        to_all([0] + within, functools.partial(send_out, result.at[f], landed.at[f, my_row], out_recv.at[f]))

    def keep(target):
        def use(here, value):
            target[:, here] = value
        return use

    def multiply(first):
        def use(here, value):
            flux[:, here] = (value * vertical[:, here]).astype(jnp.bfloat16)
            product = value * other[:, here]
            total[:, here] = product if first else total[:, here] + product
        return use

    def double(here, value):
        total[:, here] += 2.0 * value * vertical[:, here]

    def last(here, value):
        flux[:, here] = (value * vertical[:, here]).astype(jnp.bfloat16)
        summed[:, here] = (total[:, here] + value * other[:, here]).astype(jnp.bfloat16)

    table_copy.wait()
    gather(0, keep(vertical))
    gather(1, keep(other))
    gather(2, multiply(True))
    finish(0)
    gather(3, keep(other))
    gather(4, multiply(False))
    finish(1)
    gather(5, keep(other))
    gather(6, double)
    gather(7, last)
    finish(2)
    finish(3)

    def settle(f):
        wait(landed.at[f], out_recv.at[f])
        if f == 2:
            wait(crossed, cross_recv)
        for y in range(rows_y):
            value = landed[f, y].astype(jnp.float32)
            if f == 2:
                value += crossed[y].astype(jnp.float32)
            wide[pl.ds(y, local_m, stride=rows_y), :] = value

        def lay(step, carry):
            here = pl.ds(pl.multiple_of(step * chunk, chunk), chunk)
            stage[step, pl.ds(f, local_k, stride=fields), :] = wide[here, :].T
            if f == 3:
                out[step] = stage[step].astype(jnp.bfloat16)
            return carry

        lax.fori_loop(0, columns // chunk, lay, 0, unroll=f >= 2)

    for f in (0, 1, 2, 3):
        settle(f)

    wait(rows.at[pl.ds(0, fields)], in_send)
    wait(rows.at[:, pl.ds(0, rows_y - 1)], in_send)
    wait(landed.at[:, pl.ds(0, rows_y - 1)], out_send)
    wait(crossed, out_send)


def deliver(tiles, out, sem):
    for n in range(tiles.shape[0]):
        pltpu.make_async_copy(tiles.at[n], out.at[:, :, pl.ds(n * 128, 128)], sem).start()
    pltpu.make_async_copy(out, out, sem).wait()


def on_device(nkx, ncz, field_modes, cotangent):
    local_k, fields, columns = field_modes.shape
    local_m = columns // Y
    modes_z, points_x = local_k * ncz, local_m * nkx
    own_rows = Y // nkx
    share_x = points_x // ncz
    bf16 = jnp.bfloat16
    pieces = next(p for p in (3, 2, 1) if columns % (p * 16 * Y) == 0 or p == 1)

    cosines = cosine_table(MZ, modes_z)
    synthesis = (cosines * math.sqrt(2.0 / modes_z)).astype(bf16).T
    projection = (cosines * math.sqrt(2.0 / MZ)).astype(bf16).T
    hartley = hartley_table(points_x).astype(np.float32).astype(bf16)
    tables = jnp.asarray(np.concatenate([hartley, synthesis, projection], axis=0))

    hbm = pl.BlockSpec(memory_space=pltpu.HBM)
    dma = pltpu.SemaphoreType.DMA
    whole_rows = nkx // 2 * ncz == Y and nkx & (nkx - 1) == 0 and local_k % 128 == 0
    if whole_rows:
        members = nkx // 2
        body = kernel_halves
        scratch = [
            pltpu.VMEM((fields, points_x, modes_z), bf16),
            pltpu.VMEM((fields, members * local_m, modes_z), bf16),
            pltpu.VMEM((points_x, modes_z), bf16),
            pltpu.VMEM((points_x, MZ), jnp.float32),
            pltpu.VMEM((points_x, MZ), jnp.float32),
            pltpu.VMEM((points_x, MZ), jnp.float32),
            pltpu.VMEM((points_x, MZ), bf16),
            pltpu.VMEM((points_x, MZ), bf16),
            pltpu.VMEM((points_x, modes_z), bf16),
            pltpu.VMEM((fields, members * local_m, modes_z), bf16),
            pltpu.VMEM((members * local_m, modes_z), bf16),
            pltpu.VMEM((fields, Y, local_m, local_k), bf16),
            pltpu.VMEM((Y, local_m, local_k), bf16),
            dma, dma((2 * fields,)), dma, dma((fields,)), dma,
        ]
    else:
        body = kernel
        scratch = [
            pltpu.VMEM((2 * fields, own_rows, points_x, local_k), bf16),
            pltpu.VMEM((2 * fields, points_x, own_rows * local_k), bf16),
            pltpu.VMEM((2 * fields, ncz, share_x, own_rows * local_k), bf16),
            pltpu.VMEM((fields, own_rows * share_x, MZ), jnp.float32),
            pltpu.VMEM((own_rows * share_x, MZ), jnp.float32),
            pltpu.VMEM((own_rows * share_x, MZ), bf16),
            pltpu.VMEM((fields, ncz, share_x, own_rows * local_k), bf16),
            pltpu.VMEM((fields, points_x, own_rows * local_k), bf16),
            pltpu.VMEM((fields, own_rows, points_x, local_k), bf16),
            pltpu.VMEM((fields, Y, local_m, local_k), bf16),
            dma, dma((2 * fields,)), dma, dma((2 * fields,)),
            dma, dma((fields,)), dma, dma((fields,)),
        ]
    out = pl.pallas_call(
        functools.partial(body, nkx, ncz, pieces),
        out_shape=jax.ShapeDtypeStruct((columns // 128, fields * local_k, 128), bf16),
        in_specs=[hbm] * 3,
        out_specs=pl.BlockSpec(memory_space=pltpu.VMEM),
        scratch_shapes=[
            pltpu.VMEM((2, local_k, fields, columns), bf16),
            pltpu.VMEM(tables.shape, bf16),
            dma((2, pieces)), dma, pltpu.SemaphoreType.REGULAR((nkx // 2 + 1,)),
            pltpu.VMEM((16 * Y, 16 * Y), bf16),
            pltpu.VMEM((columns, local_k), jnp.float32),
            pltpu.VMEM((columns // 128, fields * local_k, 128), jnp.float32),
            pltpu.VMEM((2 * fields, Y, local_m, local_k), bf16),
            *scratch,
        ],
        compiler_params=pltpu.CompilerParams(has_side_effects=True, vmem_limit_bytes=52 * 2**20, collective_id=0),
    )(field_modes, cotangent, tables)
    return pl.pallas_call(
        deliver,
        out_shape=jax.ShapeDtypeStruct(field_modes.shape, bf16),
        in_specs=[pl.BlockSpec(memory_space=pl.ANY)],
        out_specs=hbm,
        scratch_shapes=[dma],
        compiler_params=pltpu.CompilerParams(vmem_limit_bytes=2 * 2**20),
    )(out.reshape(columns // 128, local_k, fields, 128))


def solution(mesh):
    return jax.shard_map(
        functools.partial(on_device, mesh.shape["kx"], mesh.shape["cz"]),
        mesh=mesh,
        in_specs=(P("cz", None, "kx"), P("cz", None, "kx")),
        out_specs=P("cz", None, "kx"),
        check_vma=False,
    )
```

```python
import functools
import math

import jax
import jax.numpy as jnp
import numpy as np
from jax import lax
from jax.experimental import pallas as pl
from jax.experimental.pallas import tpu as pltpu
from jax.sharding import PartitionSpec as P

MZ = 768
Y = 16
MESH = pl.DeviceIdType.MESH


def cosine_table(rows, columns):
    position = (np.arange(columns)[None, :] * (2 * np.arange(rows)[:, None] + 1)) % (4 * rows)
    return np.cos(np.pi * position / (2 * rows)).astype(np.float32)


def hartley_table(points):
    index = np.arange(points)
    phases = 2.0 * np.pi * ((index[:, None] * index[None, :]) % points) / points
    return (np.cos(phases) + np.sin(phases)) / math.sqrt(points)


def matmul(a, b):
    return jnp.dot(a, b, preferred_element_type=jnp.float32)


def matmul_t(a, b):
    return lax.dot_general(a, b, (((1,), (1,)), ((), ())), preferred_element_type=jnp.float32)


def kernel(
    nkx, ncz, pieces,
    field_modes, cotangent, tables_in,
    out,
    raw, tables, raw_sem, table_sem, ready,
    weave, wide, stage, rows, held, mixed, parts, points, total, flux, lowered, turned, result, landed,
    in_send, in_recv, swap_send, swap_recv, back_send, back_recv, out_send, out_recv,
):
    local_k, fields, columns = field_modes.shape
    rows_y = rows.shape[1]
    local_m = columns // rows_y
    own_rows = rows_y // nkx
    points_x = local_m * nkx
    points_z = points.shape[2]
    modes_z = local_k * ncz
    share_x = points_x // ncz
    aligned = local_k % 128 == 0
    i, j = lax.axis_index("kx"), lax.axis_index("cz")
    ahead = 3
    order = ((0, 2), (1, 0), (1, 1), (1, 3), (0, 0), (0, 1), (0, 3), (1, 2))

    places = nkx // 2
    place, column = i // 2, lax.rem(i, 2)
    above, below = place + 1 < places, place > 0
    inner = jnp.logical_or(place == places // 2 - 1, place == places // 2)
    near = 1 + jnp.where(above, 1, 0) + jnp.where(below, 1, 0)

    def at(row_owner, mode_owner):
        return {"kx": row_owner, "cz": mode_owner}

    def wait(ref, sem):
        pltpu.make_async_copy(ref, ref, sem).wait()

    piece = columns // pieces
    raw_copies = [
        [
            pltpu.make_async_copy(
                array.at[:, :, pl.ds(p * piece, piece)], raw.at[a, :, :, pl.ds(p * piece, piece)], raw_sem.at[a, p]
            )
            for p in range(pieces)
        ]
        for a, array in enumerate((field_modes, cotangent))
    ]
    table_copy = pltpu.make_async_copy(tables_in, tables, table_sem)
    for copy in raw_copies[0]:
        copy.start()
    barrier = pltpu.get_barrier_semaphore()

    def signal_near(sem):
        pl.semaphore_signal(sem, inc=1, device_id=at(place * 2 + 1 - column, j), device_id_type=MESH)

        @pl.when(above)
        def _():
            pl.semaphore_signal(sem, inc=1, device_id=at(i + 2, j), device_id_type=MESH)

        @pl.when(below)
        def _():
            pl.semaphore_signal(sem, inc=1, device_id=at(i - 2, j), device_id_type=MESH)

    signal_near(barrier)
    for step in range(1, ncz):
        pl.semaphore_signal(barrier, inc=1, device_id=at(i, lax.rem(j + step, ncz)), device_id_type=MESH)

    hartley = tables.at[pl.ds(0, points_x)]
    lifts = [tables.at[pl.ds(points_x + n * modes_z, modes_z)] for n in range(2)]
    chunk, group = 128, 16
    block = group * rows_y
    row = lax.broadcasted_iota(jnp.int32, (block, block), 0)
    lane = lax.broadcasted_iota(jnp.int32, (block, block), 1)
    moved = lax.rem(row, group) * rows_y + row // group
    weave[...] = jnp.where(moved == lane, 1.0, 0.0).astype(jnp.bfloat16)

    def prepare(h, between=None):
        a, f = order[h]

        def turn(step, carry):
            here = pl.ds(pl.multiple_of(step * block, block), block)
            value = matmul_t(weave[...], raw[a, :, f, here]).astype(jnp.bfloat16)
            rows[h, :, pl.ds(pl.multiple_of(step * group, group), group), :] = value.reshape(rows_y, group, local_k)
            return carry

        if h >= 2:
            lax.fori_loop(0, columns // block, turn, 0)
        else:
            span = columns // block // pieces
            for p in range(pieces):
                raw_copies[a][p].wait()
                lax.fori_loop(p * span, (p + 1) * span, turn, 0)
                if between is not None:
                    between(p)

    def in_place(h, start=0, count=local_m):
        return held.at[h, :, pl.ds(pl.multiple_of(i * local_m, local_m) + start, count)]

    def send_in(h, target, start=0, count=local_m):
        pltpu.make_async_remote_copy(
            src_ref=rows.at[h, pl.ds(target * own_rows, own_rows), pl.ds(start, count)],
            dst_ref=in_place(h, start, count),
            send_sem=in_send,
            recv_sem=in_recv.at[h],
            device_id=at(target, j),
            device_id_type=MESH,
        ).start()

    def keep_in(h):
        pltpu.make_async_copy(rows.at[h, pl.ds(i * own_rows, own_rows)], in_place(h), in_recv.at[h]).start()

    def flip(index, step):
        bit = 1
        target = index
        while bit < nkx:
            if step & bit:
                target = target + bit * (1 - 2 * lax.rem(index // bit, 2))
            bit *= 2
        return target

    half = nkx // 2
    within = list(range(1, half))
    across = [s for p in range(half // 2, places) for s in (2 * p + 1, 2 * p)]

    def targets(chosen):
        if nkx & (nkx - 1):
            return [lax.rem(i + s, nkx) for s in chosen]
        return [flip(i, s) for s in chosen]

    def send_at_distance(h, distance, start=0, count=local_m):
        for hops, side in ((distance, 0), (distance - 1, 1)):
            facing = place * 2 + (column if side == 0 else 1 - column)
            if hops == 0:
                send_in(h, facing, start, count)
            elif hops < places:
                @pl.when(place + hops < places)
                def _():
                    send_in(h, facing + 2 * hops, start, count)

                @pl.when(place >= hops)
                def _():
                    send_in(h, facing - 2 * hops, start, count)

    part_m = local_m // pieces

    def begin(p):
        if p == 0:
            pl.semaphore_wait(barrier, near + ncz - 1)
            if places > 1:
                signal_near(ready.at[0])
        if p == pieces - 1:
            for copy in raw_copies[1]:
                copy.start()
        send_at_distance(0, 1, p * part_m, part_m)

    prepare(0, begin)
    for distance in range(2, places + 1):
        pl.semaphore_wait(ready.at[distance - 2], near)
        if distance < places:
            signal_near(ready.at[distance - 1])
        send_at_distance(0, distance)
    keep_in(0)
    table_copy.start()

    def launch(h):
        if h < 2 * fields:
            prepare(h)
            for target in targets(within + across):
                send_in(h, target)
            keep_in(h)

    for h in range(1, ahead):
        launch(h)

    def share_rows(q):
        return pl.ds(pl.multiple_of(q * share_x, share_x), share_x)

    def lanes(r):
        return slice(r * local_k, (r + 1) * local_k)

    def transform(target, source):
        if aligned:
            joined = source[0] if len(source) == 1 else jnp.concatenate(source, axis=1)
            value = matmul(hartley[...], joined).astype(jnp.bfloat16)
            for r in range(own_rows):
                target(r, value[:, lanes(r)])
        else:
            for r in range(own_rows):
                target(r, matmul(hartley[...], source[r]).astype(jnp.bfloat16))

    def mix(h):
        wait(held.at[h], in_recv.at[h])

        def keep(r, value):
            mixed[h, :, lanes(r)] = value

        transform(keep, [held[h, r] for r in range(own_rows)])
        for step in range(1, ncz):
            q = lax.rem(j + step, ncz)
            pltpu.make_async_remote_copy(
                src_ref=mixed.at[h, share_rows(q), :],
                dst_ref=parts.at[h, j],
                send_sem=swap_send,
                recv_sem=swap_recv.at[h],
                device_id=at(i, q),
                device_id_type=MESH,
            ).start()
        pltpu.make_async_copy(mixed.at[h, share_rows(j), :], parts.at[h, j], swap_recv.at[h]).start()

    block_z = 256 if points_z % 256 == 0 else points_z

    def lift(h, use):
        wait(parts.at[h], swap_recv.at[h])
        table = lifts[order[h][0]]

        def one(step, carry):
            here = pl.ds(pl.multiple_of(step * block_z, block_z), block_z)
            if aligned:
                joined = jnp.concatenate(
                    [
                        jnp.concatenate([parts[h, q, :, lanes(r)] for q in range(ncz)], axis=1)
                        for r in range(own_rows)
                    ],
                    axis=0,
                )
                use(slice(None), here, matmul(joined, table[:, here]))
            else:
                for r in range(own_rows):
                    value = matmul(parts[h, 0, :, lanes(r)], table[0:local_k, here])
                    for q in range(1, ncz):
                        value += matmul(parts[h, q, :, lanes(r)], table[q * local_k:(q + 1) * local_k, here])
                    use(slice(r * share_x, (r + 1) * share_x), here, value)
            return carry

        lax.fori_loop(0, points_z // block_z, one, 0)

    def leave(f):
        if aligned:
            value = matmul_t(flux[...], lifts[0][...]).astype(jnp.bfloat16)
            for q in range(ncz):
                for r in range(own_rows):
                    lowered[f, q, :, lanes(r)] = value[r * share_x:(r + 1) * share_x, lanes(q)]
        else:
            for q in range(ncz):
                for r in range(own_rows):
                    lowered[f, q, :, lanes(r)] = matmul_t(
                        flux[r * share_x:(r + 1) * share_x, :], lifts[0][q * local_k:(q + 1) * local_k, :]
                    ).astype(jnp.bfloat16)
        for step in range(1, ncz):
            q = lax.rem(j + step, ncz)
            pltpu.make_async_remote_copy(
                src_ref=lowered.at[f, q],
                dst_ref=turned.at[f, share_rows(j), :],
                send_sem=back_send,
                recv_sem=back_recv.at[f],
                device_id=at(i, q),
                device_id_type=MESH,
            ).start()
        pltpu.make_async_copy(lowered.at[f, j], turned.at[f, share_rows(j), :], back_recv.at[f]).start()

    def out_block(f, target):
        return result.at[f, :, pl.ds(pl.multiple_of(target * local_m, local_m), local_m)]

    def out_place(f):
        return landed.at[f, pl.ds(i * own_rows, own_rows)]

    def finish(f):
        wait(turned.at[f], back_recv.at[f])

        def keep(r, value):
            result[f, r] = value

        transform(keep, [turned[f, :, lanes(r)] for r in range(own_rows)])
        pltpu.make_async_copy(out_block(f, i), out_place(f), out_recv.at[f]).start()

    def depart(f, chosen):
        for target in targets(chosen):
            pltpu.make_async_remote_copy(
                src_ref=out_block(f, target),
                dst_ref=out_place(f),
                send_sem=out_send,
                recv_sem=out_recv.at[f],
                device_id=at(target, j),
                device_id_type=MESH,
            ).start()

    outer = jnp.logical_not(inner)

    def settle(f):
        wait(landed.at[f], out_recv.at[f])
        for y in range(rows_y):
            wide[pl.ds(y, local_m, stride=rows_y), :] = landed[f, y].astype(jnp.float32)

        def lay(step, carry):
            here = pl.ds(pl.multiple_of(step * chunk, chunk), chunk)
            stage[step, pl.ds(f, local_k, stride=fields), :] = wide[here, :].T
            if f == 2:
                out[step] = stage[step].astype(jnp.bfloat16)
            return carry

        lax.fori_loop(0, columns // chunk, lay, 0, unroll=f in (2, 3))

    def keep(h):
        def use(part, here, value):
            points[h, part, here] = value
        return use

    def keep_and_flux(h):
        def use(part, here, value):
            points[h, part, here] = value
            flux[part, here] = (value * points[0, part, here]).astype(jnp.bfloat16)
        return use

    def first(part, here, value):
        total[part, here] = points[1, part, here] * value

    def add(h):
        def use(part, here, value):
            total[part, here] += points[h, part, here] * value
        return use

    def last(part, here, value):
        flux[part, here] = (total[part, here] + 2.0 * value * points[0, part, here]).astype(jnp.bfloat16)

    table_copy.wait()
    mix(0)
    launch(ahead)
    mix(1)
    launch(ahead + 1)
    lift(0, keep(0))
    mix(2)
    launch(ahead + 2)
    lift(1, keep_and_flux(1))
    leave(0)
    mix(3)
    launch(ahead + 3)
    lift(2, keep_and_flux(2))
    leave(1)
    finish(0)
    mix(4)
    launch(ahead + 4)
    lift(3, keep_and_flux(3))
    leave(3)
    finish(1)

    @pl.when(inner)
    def _():
        depart(0, within + across)
        depart(1, within + across)

    mix(5)
    launch(ahead + 5)
    lift(4, first)
    finish(3)

    @pl.when(inner)
    def _():
        depart(3, within + across)

    mix(6)
    launch(ahead + 6)
    lift(5, add(2))
    mix(7)

    @pl.when(outer)
    def _():
        for f in (0, 1, 3):
            depart(f, within + across)

    lift(6, add(3))
    lift(7, last)
    leave(2)
    finish(2)
    depart(2, within + across)

    for f in (0, 1, 3, 2):
        settle(f)

    wait(rows.at[:, pl.ds(0, rows_y - own_rows)], in_send)
    wait(mixed.at[:, pl.ds(0, points_x - share_x), :], swap_send)
    wait(lowered.at[:, pl.ds(0, ncz - 1)], back_send)
    wait(landed.at[:, pl.ds(0, rows_y - own_rows)], out_send)


def kernel_halves(
    nkx, ncz, pieces,
    field_modes, cotangent, tables_in,
    out,
    raw, tables, raw_sem, table_sem, ready,
    weave, wide, stage, rows, held, kept, mixed, vertical, other, total, flux, summed, lowered, result, beyond, landed, crossed,
    in_send, in_recv, out_send, out_recv, cross_recv,
):
    local_k, fields, columns = field_modes.shape
    rows_y = rows.shape[1]
    local_m = columns // rows_y
    points_x = local_m * nkx
    points_z = vertical.shape[1]
    modes_z = local_k * ncz
    members = nkx // 2
    half_m = members * local_m
    i, j = lax.axis_index("kx"), lax.axis_index("cz")
    side, member = i // members, lax.rem(i, members)
    my_row = member * ncz + j
    order = ((0, 2), (0, 0), (1, 0), (0, 1), (1, 1), (0, 3), (1, 2), (1, 3))
    shared = (True, False, True, False, True, False, False, True)
    place_of = [sum(shared[:h]) if shared[h] else h - sum(shared[:h]) for h in range(2 * fields)]
    ahead = 6

    places = nkx // 2
    place, column = i // 2, lax.rem(i, 2)
    above, below = place + 1 < places, place > 0
    near = ncz + jnp.where(above, 1, 0) + jnp.where(below, 1, 0)

    def at(row_owner, mode_owner):
        return {"kx": row_owner, "cz": mode_owner}

    def wait(ref, sem):
        pltpu.make_async_copy(ref, ref, sem).wait()

    piece = columns // pieces
    raw_copies = [
        [
            pltpu.make_async_copy(
                array.at[:, :, pl.ds(p * piece, piece)], raw.at[a, :, :, pl.ds(p * piece, piece)], raw_sem.at[a, p]
            )
            for p in range(pieces)
        ]
        for a, array in enumerate((field_modes, cotangent))
    ]
    table_copy = pltpu.make_async_copy(tables_in, tables, table_sem)
    for copy in raw_copies[0]:
        copy.start()
    barrier = pltpu.get_barrier_semaphore()

    def signal_near(sem):
        pl.semaphore_signal(sem, inc=1, device_id=at(place * 2 + 1 - column, j), device_id_type=MESH)

        @pl.when(above)
        def _():
            pl.semaphore_signal(sem, inc=1, device_id=at(i + 2, j), device_id_type=MESH)

        @pl.when(below)
        def _():
            pl.semaphore_signal(sem, inc=1, device_id=at(i - 2, j), device_id_type=MESH)

        for step in range(1, ncz):
            pl.semaphore_signal(sem, inc=1, device_id=at(i, lax.rem(j + step, ncz)), device_id_type=MESH)

    signal_near(barrier)
    hartley = tables.at[pl.ds(0, points_x)]
    lifts = [tables.at[pl.ds(points_x + n * modes_z, modes_z)] for n in range(2)]
    chunk, group = 128, 16
    block = group * rows_y
    row = lax.broadcasted_iota(jnp.int32, (block, block), 0)
    lane = lax.broadcasted_iota(jnp.int32, (block, block), 1)
    moved = lax.rem(row, group) * rows_y + row // group
    weave[...] = jnp.where(moved == lane, 1.0, 0.0).astype(jnp.bfloat16)

    def prepare(h, between=None):
        a, f = order[h]

        def turn(step, carry):
            here = pl.ds(pl.multiple_of(step * block, block), block)
            value = matmul_t(weave[...], raw[a, :, f, here]).astype(jnp.bfloat16)
            rows[h, :, pl.ds(pl.multiple_of(step * group, group), group), :] = value.reshape(rows_y, group, local_k)
            return carry

        if all(order[n][0] != a for n in range(h)):
            span = columns // block // pieces
            for p in range(pieces):
                raw_copies[a][p].wait()
                lax.fori_loop(p * span, (p + 1) * span, turn, 0)
                if between is not None:
                    between(p)
        else:
            lax.fori_loop(0, columns // block, turn, 0)

    my_lanes = pl.ds(pl.multiple_of(j * local_k, local_k), local_k)

    def in_place(h, start=0, count=local_m):
        if shared[h]:
            return held.at[place_of[h], pl.ds(pl.multiple_of(i * local_m, local_m) + start, count), my_lanes]
        return kept.at[place_of[h], pl.ds(pl.multiple_of(member * local_m, local_m) + start, count), my_lanes]

    def send_in(h, row_owner, mode_owner, start=0, count=local_m):
        pltpu.make_async_remote_copy(
            src_ref=rows.at[h, lax.rem(row_owner, members) * ncz + mode_owner, pl.ds(start, count)],
            dst_ref=in_place(h, start, count),
            send_sem=in_send,
            recv_sem=in_recv.at[h],
            device_id=at(row_owner, mode_owner),
            device_id_type=MESH,
        ).start()

    def keep_in(h):
        pltpu.make_async_copy(rows.at[h, my_row], in_place(h), in_recv.at[h]).start()

    def flip(index, step):
        bit = 1
        target = index
        while bit < nkx:
            if step & bit:
                target = target + bit * (1 - 2 * lax.rem(index // bit, 2))
            bit *= 2
        return target

    within = list(range(1, members))
    across = [s for p in range(places - 1, members // 2 - 1, -1) for s in (2 * p + 1, 2 * p)]

    def to_all(steps, send):
        def one(step, carry):
            for s in steps:
                if s:
                    send(flip(i, s), lax.rem(j + step, ncz))
                else:
                    @pl.when(step > 0)
                    def _():
                        send(i, lax.rem(j + step, ncz))
            return carry

        lax.fori_loop(0, ncz, one, 0)

    def hop_away(hops, side_step, use):
        facing = place * 2 + (1 - column if side_step else column)
        if hops == 0:
            use(facing)
        elif hops < places:
            @pl.when(place + hops < places)
            def _():
                use(facing + 2 * hops)

            @pl.when(place >= hops)
            def _():
                use(facing - 2 * hops)

    def each_other(send, target):
        def one(step, carry):
            send(target, lax.rem(j + step, ncz))
            return carry

        lax.fori_loop(1, ncz, one, 0)

    part_m = local_m // pieces

    def begin(p):
        if p == 0:
            pl.semaphore_wait(barrier, near)
            signal_near(ready.at[0])
        if p == pieces - 1:
            for copy in raw_copies[1]:
                copy.start()
        hop_away(1, False, lambda t: send_in(0, t, j, p * part_m, part_m))
        hop_away(0, True, lambda t: send_in(0, t, j, p * part_m, part_m))

    prepare(0, begin)
    send_0 = functools.partial(send_in, 0)
    each_other(send_0, i)
    for distance in range(2, places + 2):
        pl.semaphore_wait(ready.at[distance - 2], near)
        if distance < places + 1:
            signal_near(ready.at[distance - 1])
        if distance <= places:
            hop_away(distance, False, lambda t: send_in(0, t, j))
            hop_away(distance - 1, True, lambda t: send_in(0, t, j))
        hop_away(distance - 1, False, lambda t: each_other(send_0, t))
        hop_away(distance - 2, True, lambda t: each_other(send_0, t))
    keep_in(0)
    table_copy.start()

    def launch(h):
        if h < 2 * fields:
            prepare(h)
            to_all((across if shared[h] else []) + [0] + within, functools.partial(send_in, h))
            keep_in(h)

    for h in range(1, ahead):
        launch(h)

    half_lanes = modes_z // 2
    parts = [slice(n * half_lanes, (n + 1) * half_lanes) for n in range(2)]
    block_z = 256 if points_z % 256 == 0 else points_z

    def own_m(which):
        return pl.ds(pl.multiple_of(which * half_m, half_m), half_m)

    def gather(h, use):
        source = held.at[place_of[h]] if shared[h] else kept.at[place_of[h]]
        wait(source, in_recv.at[h])
        for part in parts:
            table = hartley[...] if shared[h] else hartley[:, own_m(side)]
            mixed[:, part] = matmul(table, source[:, part]).astype(jnp.bfloat16)
        launch(h + ahead)
        lift_table = lifts[order[h][0]]

        def one(step, carry):
            here = pl.ds(pl.multiple_of(step * block_z, block_z), block_z)
            use(here, matmul(mixed[...], lift_table[:, here]))
            return carry

        lax.fori_loop(0, points_z // block_z, one, 0)

    def lower(source):
        for part in parts:
            lowered[:, part] = matmul_t(source[...], lifts[0][part, :]).astype(jnp.bfloat16)

    def out_block(ref, row_owner, mode_owner):
        first_m = pl.multiple_of(lax.rem(row_owner, members) * local_m, local_m)
        return ref.at[pl.ds(first_m, local_m), pl.ds(pl.multiple_of(mode_owner * local_k, local_k), local_k)]

    def send_out(source, target, sem, row_owner, mode_owner):
        pltpu.make_async_remote_copy(
            src_ref=out_block(source, row_owner, mode_owner),
            dst_ref=target,
            send_sem=out_send,
            recv_sem=sem,
            device_id=at(row_owner, mode_owner),
            device_id_type=MESH,
        ).start()

    def finish(f):
        lower(summed if f == 2 else flux)
        if f == 2:
            for part in parts:
                beyond[:, part] = matmul(hartley[own_m(1 - side), :], lowered[:, part]).astype(jnp.bfloat16)
            to_all(across, functools.partial(send_out, beyond, crossed.at[my_row], cross_recv))
        for part in parts:
            result[f, :, part] = matmul(hartley[own_m(side), :], lowered[:, part]).astype(jnp.bfloat16)
        pltpu.make_async_copy(out_block(result.at[f], i, j), landed.at[f, my_row], out_recv.at[f]).start()
        to_all([0] + within, functools.partial(send_out, result.at[f], landed.at[f, my_row], out_recv.at[f]))

    def keep(target):
        def use(here, value):
            target[:, here] = value
        return use

    def multiply(first):
        def use(here, value):
            flux[:, here] = (value * vertical[:, here]).astype(jnp.bfloat16)
            product = value * other[:, here]
            total[:, here] = product if first else total[:, here] + product
        return use

    def double(here, value):
        total[:, here] += 2.0 * value * vertical[:, here]

    def last(here, value):
        flux[:, here] = (value * vertical[:, here]).astype(jnp.bfloat16)
        summed[:, here] = (total[:, here] + value * other[:, here]).astype(jnp.bfloat16)

    table_copy.wait()
    gather(0, keep(vertical))
    gather(1, keep(other))
    gather(2, multiply(True))
    finish(0)
    gather(3, keep(other))
    gather(4, multiply(False))
    finish(1)
    gather(5, keep(other))
    gather(6, double)
    gather(7, last)
    finish(2)
    finish(3)

    def settle(f):
        wait(landed.at[f], out_recv.at[f])
        if f == 2:
            wait(crossed, cross_recv)
        for y in range(rows_y):
            value = landed[f, y].astype(jnp.float32)
            if f == 2:
                value += crossed[y].astype(jnp.float32)
            wide[pl.ds(y, local_m, stride=rows_y), :] = value

        def lay(step, carry):
            here = pl.ds(pl.multiple_of(step * chunk, chunk), chunk)
            stage[step, pl.ds(f, local_k, stride=fields), :] = wide[here, :].T
            if f == 3:
                out[step] = stage[step].astype(jnp.bfloat16)
            return carry

        lax.fori_loop(0, columns // chunk, lay, 0, unroll=f == 3)

    for f in (0, 1, 2, 3):
        settle(f)

    wait(rows.at[pl.ds(0, fields)], in_send)
    wait(rows.at[:, pl.ds(0, rows_y - 1)], in_send)
    wait(landed.at[:, pl.ds(0, rows_y - 1)], out_send)
    wait(crossed, out_send)


def deliver(tiles, out, sem):
    for n in range(tiles.shape[0]):
        pltpu.make_async_copy(tiles.at[n], out.at[:, :, pl.ds(n * 128, 128)], sem).start()
    pltpu.make_async_copy(out, out, sem).wait()


def on_device(nkx, ncz, field_modes, cotangent):
    local_k, fields, columns = field_modes.shape
    local_m = columns // Y
    modes_z, points_x = local_k * ncz, local_m * nkx
    own_rows = Y // nkx
    share_x = points_x // ncz
    bf16 = jnp.bfloat16
    pieces = next(p for p in (3, 2, 1) if columns % (p * 16 * Y) == 0 or p == 1)

    cosines = cosine_table(MZ, modes_z)
    synthesis = (cosines * math.sqrt(2.0 / modes_z)).astype(bf16).T
    projection = (cosines * math.sqrt(2.0 / MZ)).astype(bf16).T
    hartley = hartley_table(points_x).astype(np.float32).astype(bf16)
    tables = jnp.asarray(np.concatenate([hartley, synthesis, projection], axis=0))

    hbm = pl.BlockSpec(memory_space=pltpu.HBM)
    dma = pltpu.SemaphoreType.DMA
    whole_rows = nkx // 2 * ncz == Y and nkx & (nkx - 1) == 0 and local_k % 128 == 0
    if whole_rows:
        members = nkx // 2
        body = kernel_halves
        scratch = [
            pltpu.VMEM((fields, points_x, modes_z), bf16),
            pltpu.VMEM((fields, members * local_m, modes_z), bf16),
            pltpu.VMEM((points_x, modes_z), bf16),
            pltpu.VMEM((points_x, MZ), jnp.float32),
            pltpu.VMEM((points_x, MZ), jnp.float32),
            pltpu.VMEM((points_x, MZ), jnp.float32),
            pltpu.VMEM((points_x, MZ), bf16),
            pltpu.VMEM((points_x, MZ), bf16),
            pltpu.VMEM((points_x, modes_z), bf16),
            pltpu.VMEM((fields, members * local_m, modes_z), bf16),
            pltpu.VMEM((members * local_m, modes_z), bf16),
            pltpu.VMEM((fields, Y, local_m, local_k), bf16),
            pltpu.VMEM((Y, local_m, local_k), bf16),
            dma, dma((2 * fields,)), dma, dma((fields,)), dma,
        ]
    else:
        body = kernel
        scratch = [
            pltpu.VMEM((2 * fields, own_rows, points_x, local_k), bf16),
            pltpu.VMEM((2 * fields, points_x, own_rows * local_k), bf16),
            pltpu.VMEM((2 * fields, ncz, share_x, own_rows * local_k), bf16),
            pltpu.VMEM((fields, own_rows * share_x, MZ), jnp.float32),
            pltpu.VMEM((own_rows * share_x, MZ), jnp.float32),
            pltpu.VMEM((own_rows * share_x, MZ), bf16),
            pltpu.VMEM((fields, ncz, share_x, own_rows * local_k), bf16),
            pltpu.VMEM((fields, points_x, own_rows * local_k), bf16),
            pltpu.VMEM((fields, own_rows, points_x, local_k), bf16),
            pltpu.VMEM((fields, Y, local_m, local_k), bf16),
            dma, dma((2 * fields,)), dma, dma((2 * fields,)),
            dma, dma((fields,)), dma, dma((fields,)),
        ]
    out = pl.pallas_call(
        functools.partial(body, nkx, ncz, pieces),
        out_shape=jax.ShapeDtypeStruct((columns // 128, fields * local_k, 128), bf16),
        in_specs=[hbm] * 3,
        out_specs=pl.BlockSpec(memory_space=pltpu.VMEM),
        scratch_shapes=[
            pltpu.VMEM((2, local_k, fields, columns), bf16),
            pltpu.VMEM(tables.shape, bf16),
            dma((2, pieces)), dma, pltpu.SemaphoreType.REGULAR((nkx // 2 + 1,)),
            pltpu.VMEM((16 * Y, 16 * Y), bf16),
            pltpu.VMEM((columns, local_k), jnp.float32),
            pltpu.VMEM((columns // 128, fields * local_k, 128), jnp.float32),
            pltpu.VMEM((2 * fields, Y, local_m, local_k), bf16),
            *scratch,
        ],
        compiler_params=pltpu.CompilerParams(has_side_effects=True, vmem_limit_bytes=52 * 2**20, collective_id=0),
    )(field_modes, cotangent, tables)
    return pl.pallas_call(
        deliver,
        out_shape=jax.ShapeDtypeStruct(field_modes.shape, bf16),
        in_specs=[pl.BlockSpec(memory_space=pl.ANY)],
        out_specs=hbm,
        scratch_shapes=[dma],
        compiler_params=pltpu.CompilerParams(vmem_limit_bytes=2 * 2**20),
    )(out.reshape(columns // 128, local_k, fields, 128))


def solution(mesh):
    return jax.shard_map(
        functools.partial(on_device, mesh.shape["kx"], mesh.shape["cz"]),
        mesh=mesh,
        in_specs=(P("cz", None, "kx"), P("cz", None, "kx")),
        out_specs=P("cz", None, "kx"),
        check_vma=False,
    )
```

```python
import functools
import math

import jax
import jax.numpy as jnp
import numpy as np
from jax import lax
from jax.experimental import pallas as pl
from jax.experimental.pallas import tpu as pltpu
from jax.sharding import PartitionSpec as P

MZ = 768
Y = 16
MESH = pl.DeviceIdType.MESH


def cosine_table(rows, columns):
    position = (np.arange(columns)[None, :] * (2 * np.arange(rows)[:, None] + 1)) % (4 * rows)
    return np.cos(np.pi * position / (2 * rows)).astype(np.float32)


def hartley_table(points):
    index = np.arange(points)
    phases = 2.0 * np.pi * ((index[:, None] * index[None, :]) % points) / points
    return (np.cos(phases) + np.sin(phases)) / math.sqrt(points)


def matmul(a, b):
    return jnp.dot(a, b, preferred_element_type=jnp.float32)


def matmul_t(a, b):
    return lax.dot_general(a, b, (((1,), (1,)), ((), ())), preferred_element_type=jnp.float32)


def kernel(
    nkx, ncz, pieces,
    field_modes, cotangent, tables_in,
    out,
    raw, tables, raw_sem, table_sem, ready,
    weave, wide, stage, rows, held, mixed, parts, points, total, flux, lowered, turned, result, landed,
    in_send, in_recv, swap_send, swap_recv, back_send, back_recv, out_send, out_recv,
):
    local_k, fields, columns = field_modes.shape
    rows_y = rows.shape[1]
    local_m = columns // rows_y
    own_rows = rows_y // nkx
    points_x = local_m * nkx
    points_z = points.shape[2]
    modes_z = local_k * ncz
    share_x = points_x // ncz
    aligned = local_k % 128 == 0
    i, j = lax.axis_index("kx"), lax.axis_index("cz")
    ahead = 3
    order = ((0, 2), (1, 0), (1, 1), (1, 3), (0, 0), (0, 1), (0, 3), (1, 2))

    places = nkx // 2
    place, column = i // 2, lax.rem(i, 2)
    above, below = place + 1 < places, place > 0
    inner = jnp.logical_or(place == places // 2 - 1, place == places // 2)
    near = 1 + jnp.where(above, 1, 0) + jnp.where(below, 1, 0)

    def at(row_owner, mode_owner):
        return {"kx": row_owner, "cz": mode_owner}

    def wait(ref, sem):
        pltpu.make_async_copy(ref, ref, sem).wait()

    piece = columns // pieces
    raw_copies = [
        [
            pltpu.make_async_copy(
                array.at[:, :, pl.ds(p * piece, piece)], raw.at[a, :, :, pl.ds(p * piece, piece)], raw_sem.at[a, p]
            )
            for p in range(pieces)
        ]
        for a, array in enumerate((field_modes, cotangent))
    ]
    table_copy = pltpu.make_async_copy(tables_in, tables, table_sem)
    for copy in raw_copies[0]:
        copy.start()
    barrier = pltpu.get_barrier_semaphore()

    def signal_near(sem):
        pl.semaphore_signal(sem, inc=1, device_id=at(place * 2 + 1 - column, j), device_id_type=MESH)

        @pl.when(above)
        def _():
            pl.semaphore_signal(sem, inc=1, device_id=at(i + 2, j), device_id_type=MESH)

        @pl.when(below)
        def _():
            pl.semaphore_signal(sem, inc=1, device_id=at(i - 2, j), device_id_type=MESH)

    signal_near(barrier)
    for step in range(1, ncz):
        pl.semaphore_signal(barrier, inc=1, device_id=at(i, lax.rem(j + step, ncz)), device_id_type=MESH)

    hartley = tables.at[pl.ds(0, points_x)]
    lifts = [tables.at[pl.ds(points_x + n * modes_z, modes_z)] for n in range(2)]
    chunk, group = 128, 16
    block = group * rows_y
    row = lax.broadcasted_iota(jnp.int32, (block, block), 0)
    lane = lax.broadcasted_iota(jnp.int32, (block, block), 1)
    moved = lax.rem(row, group) * rows_y + row // group
    weave[...] = jnp.where(moved == lane, 1.0, 0.0).astype(jnp.bfloat16)

    def prepare(h, between=None):
        a, f = order[h]

        def turn(step, carry):
            here = pl.ds(pl.multiple_of(step * block, block), block)
            value = matmul_t(weave[...], raw[a, :, f, here]).astype(jnp.bfloat16)
            rows[h, :, pl.ds(pl.multiple_of(step * group, group), group), :] = value.reshape(rows_y, group, local_k)
            return carry

        if h >= 2:
            lax.fori_loop(0, columns // block, turn, 0)
        else:
            span = columns // block // pieces
            for p in range(pieces):
                raw_copies[a][p].wait()
                lax.fori_loop(p * span, (p + 1) * span, turn, 0)
                if between is not None:
                    between(p)

    def in_place(h, start=0, count=local_m):
        return held.at[h, :, pl.ds(pl.multiple_of(i * local_m, local_m) + start, count)]

    def send_in(h, target, start=0, count=local_m):
        pltpu.make_async_remote_copy(
            src_ref=rows.at[h, pl.ds(target * own_rows, own_rows), pl.ds(start, count)],
            dst_ref=in_place(h, start, count),
            send_sem=in_send,
            recv_sem=in_recv.at[h],
            device_id=at(target, j),
            device_id_type=MESH,
        ).start()

    def keep_in(h):
        pltpu.make_async_copy(rows.at[h, pl.ds(i * own_rows, own_rows)], in_place(h), in_recv.at[h]).start()

    def flip(index, step):
        bit = 1
        target = index
        while bit < nkx:
            if step & bit:
                target = target + bit * (1 - 2 * lax.rem(index // bit, 2))
            bit *= 2
        return target

    half = nkx // 2
    within = list(range(1, half))
    across = [s for p in range(half // 2, places) for s in (2 * p + 1, 2 * p)]

    def targets(chosen):
        if nkx & (nkx - 1):
            return [lax.rem(i + s, nkx) for s in chosen]
        return [flip(i, s) for s in chosen]

    def send_at_distance(h, distance, start=0, count=local_m):
        for hops, side in ((distance, 0), (distance - 1, 1)):
            facing = place * 2 + (column if side == 0 else 1 - column)
            if hops == 0:
                send_in(h, facing, start, count)
            elif hops < places:
                @pl.when(place + hops < places)
                def _():
                    send_in(h, facing + 2 * hops, start, count)

                @pl.when(place >= hops)
                def _():
                    send_in(h, facing - 2 * hops, start, count)

    part_m = local_m // pieces

    def begin(p):
        if p == 0:
            pl.semaphore_wait(barrier, near + ncz - 1)
            if places > 1:
                signal_near(ready.at[0])
        if p == pieces - 1:
            for copy in raw_copies[1]:
                copy.start()
        send_at_distance(0, 1, p * part_m, part_m)

    prepare(0, begin)
    for distance in range(2, places + 1):
        pl.semaphore_wait(ready.at[distance - 2], near)
        if distance < places:
            signal_near(ready.at[distance - 1])
        send_at_distance(0, distance)
    keep_in(0)
    table_copy.start()

    def launch(h):
        if h < 2 * fields:
            prepare(h)
            for target in targets(within + across):
                send_in(h, target)
            keep_in(h)

    for h in range(1, ahead):
        launch(h)

    def share_rows(q):
        return pl.ds(pl.multiple_of(q * share_x, share_x), share_x)

    def lanes(r):
        return slice(r * local_k, (r + 1) * local_k)

    def transform(target, source):
        if aligned:
            joined = source[0] if len(source) == 1 else jnp.concatenate(source, axis=1)
            value = matmul(hartley[...], joined).astype(jnp.bfloat16)
            for r in range(own_rows):
                target(r, value[:, lanes(r)])
        else:
            for r in range(own_rows):
                target(r, matmul(hartley[...], source[r]).astype(jnp.bfloat16))

    def mix(h):
        wait(held.at[h], in_recv.at[h])

        def keep(r, value):
            mixed[h, :, lanes(r)] = value

        transform(keep, [held[h, r] for r in range(own_rows)])
        for step in range(1, ncz):
            q = lax.rem(j + step, ncz)
            pltpu.make_async_remote_copy(
                src_ref=mixed.at[h, share_rows(q), :],
                dst_ref=parts.at[h, j],
                send_sem=swap_send,
                recv_sem=swap_recv.at[h],
                device_id=at(i, q),
                device_id_type=MESH,
            ).start()
        pltpu.make_async_copy(mixed.at[h, share_rows(j), :], parts.at[h, j], swap_recv.at[h]).start()

    block_z = 256 if points_z % 256 == 0 else points_z

    def lift(h, use):
        wait(parts.at[h], swap_recv.at[h])
        table = lifts[order[h][0]]

        def one(step, carry):
            here = pl.ds(pl.multiple_of(step * block_z, block_z), block_z)
            if aligned:
                joined = jnp.concatenate(
                    [
                        jnp.concatenate([parts[h, q, :, lanes(r)] for q in range(ncz)], axis=1)
                        for r in range(own_rows)
                    ],
                    axis=0,
                )
                use(slice(None), here, matmul(joined, table[:, here]))
            else:
                for r in range(own_rows):
                    value = matmul(parts[h, 0, :, lanes(r)], table[0:local_k, here])
                    for q in range(1, ncz):
                        value += matmul(parts[h, q, :, lanes(r)], table[q * local_k:(q + 1) * local_k, here])
                    use(slice(r * share_x, (r + 1) * share_x), here, value)
            return carry

        lax.fori_loop(0, points_z // block_z, one, 0)

    def leave(f):
        if aligned:
            value = matmul_t(flux[...], lifts[0][...]).astype(jnp.bfloat16)
            for q in range(ncz):
                for r in range(own_rows):
                    lowered[f, q, :, lanes(r)] = value[r * share_x:(r + 1) * share_x, lanes(q)]
        else:
            for q in range(ncz):
                for r in range(own_rows):
                    lowered[f, q, :, lanes(r)] = matmul_t(
                        flux[r * share_x:(r + 1) * share_x, :], lifts[0][q * local_k:(q + 1) * local_k, :]
                    ).astype(jnp.bfloat16)
        for step in range(1, ncz):
            q = lax.rem(j + step, ncz)
            pltpu.make_async_remote_copy(
                src_ref=lowered.at[f, q],
                dst_ref=turned.at[f, share_rows(j), :],
                send_sem=back_send,
                recv_sem=back_recv.at[f],
                device_id=at(i, q),
                device_id_type=MESH,
            ).start()
        pltpu.make_async_copy(lowered.at[f, j], turned.at[f, share_rows(j), :], back_recv.at[f]).start()

    def out_block(f, target):
        return result.at[f, :, pl.ds(pl.multiple_of(target * local_m, local_m), local_m)]

    def out_place(f):
        return landed.at[f, pl.ds(i * own_rows, own_rows)]

    def finish(f):
        wait(turned.at[f], back_recv.at[f])

        def keep(r, value):
            result[f, r] = value

        transform(keep, [turned[f, :, lanes(r)] for r in range(own_rows)])
        pltpu.make_async_copy(out_block(f, i), out_place(f), out_recv.at[f]).start()

    def depart(f, chosen):
        for target in targets(chosen):
            pltpu.make_async_remote_copy(
                src_ref=out_block(f, target),
                dst_ref=out_place(f),
                send_sem=out_send,
                recv_sem=out_recv.at[f],
                device_id=at(target, j),
                device_id_type=MESH,
            ).start()

    outer = jnp.logical_not(inner)

    def settle(f):
        wait(landed.at[f], out_recv.at[f])
        for y in range(rows_y):
            wide[pl.ds(y, local_m, stride=rows_y), :] = landed[f, y].astype(jnp.float32)

        def lay(step, carry):
            here = pl.ds(pl.multiple_of(step * chunk, chunk), chunk)
            stage[step, pl.ds(f, local_k, stride=fields), :] = wide[here, :].T
            if f == 2:
                out[step] = stage[step].astype(jnp.bfloat16)
            return carry

        lax.fori_loop(0, columns // chunk, lay, 0, unroll=f in (2, 3))

    def keep(h):
        def use(part, here, value):
            points[h, part, here] = value
        return use

    def keep_and_flux(h):
        def use(part, here, value):
            points[h, part, here] = value
            flux[part, here] = (value * points[0, part, here]).astype(jnp.bfloat16)
        return use

    def first(part, here, value):
        total[part, here] = points[1, part, here] * value

    def add(h):
        def use(part, here, value):
            total[part, here] += points[h, part, here] * value
        return use

    def last(part, here, value):
        flux[part, here] = (total[part, here] + 2.0 * value * points[0, part, here]).astype(jnp.bfloat16)

    table_copy.wait()
    mix(0)
    launch(ahead)
    mix(1)
    launch(ahead + 1)
    lift(0, keep(0))
    mix(2)
    launch(ahead + 2)
    lift(1, keep_and_flux(1))
    leave(0)
    mix(3)
    launch(ahead + 3)
    lift(2, keep_and_flux(2))
    leave(1)
    finish(0)
    mix(4)
    launch(ahead + 4)
    lift(3, keep_and_flux(3))
    leave(3)
    finish(1)

    @pl.when(inner)
    def _():
        depart(0, within + across)
        depart(1, within + across)

    mix(5)
    launch(ahead + 5)
    lift(4, first)
    finish(3)

    @pl.when(inner)
    def _():
        depart(3, within + across)

    mix(6)
    launch(ahead + 6)
    lift(5, add(2))
    mix(7)

    @pl.when(outer)
    def _():
        for f in (0, 1, 3):
            depart(f, within + across)

    lift(6, add(3))
    lift(7, last)
    leave(2)
    finish(2)
    depart(2, within + across)

    for f in (0, 1, 3, 2):
        settle(f)

    wait(rows.at[:, pl.ds(0, rows_y - own_rows)], in_send)
    wait(mixed.at[:, pl.ds(0, points_x - share_x), :], swap_send)
    wait(lowered.at[:, pl.ds(0, ncz - 1)], back_send)
    wait(landed.at[:, pl.ds(0, rows_y - own_rows)], out_send)


def kernel_halves(
    nkx, ncz, pieces,
    field_modes, cotangent, tables_in,
    out,
    raw, tables, raw_sem, table_sem, ready,
    weave, wide, stage, rows, held, kept, mixed, vertical, other, total, flux, summed, lowered, result, beyond, landed, crossed,
    in_send, in_recv, out_send, out_recv, cross_recv,
):
    local_k, fields, columns = field_modes.shape
    rows_y = rows.shape[1]
    local_m = columns // rows_y
    points_x = local_m * nkx
    points_z = vertical.shape[1]
    modes_z = local_k * ncz
    members = nkx // 2
    half_m = members * local_m
    i, j = lax.axis_index("kx"), lax.axis_index("cz")
    side, member = i // members, lax.rem(i, members)
    my_row = member * ncz + j
    order = ((0, 2), (0, 0), (1, 0), (0, 1), (1, 1), (0, 3), (1, 2), (1, 3))
    shared = (True, False, True, False, True, False, False, True)
    place_of = [sum(shared[:h]) if shared[h] else h - sum(shared[:h]) for h in range(2 * fields)]
    ahead = 8

    places = nkx // 2
    place, column = i // 2, lax.rem(i, 2)
    above, below = place + 1 < places, place > 0
    near = ncz + jnp.where(above, 1, 0) + jnp.where(below, 1, 0)

    def at(row_owner, mode_owner):
        return {"kx": row_owner, "cz": mode_owner}

    def wait(ref, sem):
        pltpu.make_async_copy(ref, ref, sem).wait()

    piece = columns // pieces
    raw_copies = [
        [
            pltpu.make_async_copy(
                array.at[:, :, pl.ds(p * piece, piece)], raw.at[a, :, :, pl.ds(p * piece, piece)], raw_sem.at[a, p]
            )
            for p in range(pieces)
        ]
        for a, array in enumerate((field_modes, cotangent))
    ]
    table_copy = pltpu.make_async_copy(tables_in, tables, table_sem)
    for copy in raw_copies[0]:
        copy.start()
    barrier = pltpu.get_barrier_semaphore()

    def signal_near(sem):
        pl.semaphore_signal(sem, inc=1, device_id=at(place * 2 + 1 - column, j), device_id_type=MESH)

        @pl.when(above)
        def _():
            pl.semaphore_signal(sem, inc=1, device_id=at(i + 2, j), device_id_type=MESH)

        @pl.when(below)
        def _():
            pl.semaphore_signal(sem, inc=1, device_id=at(i - 2, j), device_id_type=MESH)

        for step in range(1, ncz):
            pl.semaphore_signal(sem, inc=1, device_id=at(i, lax.rem(j + step, ncz)), device_id_type=MESH)

    signal_near(barrier)
    hartley = tables.at[pl.ds(0, points_x)]
    lifts = [tables.at[pl.ds(points_x + n * modes_z, modes_z)] for n in range(2)]
    chunk, group = 128, 16
    block = group * rows_y
    row = lax.broadcasted_iota(jnp.int32, (block, block), 0)
    lane = lax.broadcasted_iota(jnp.int32, (block, block), 1)
    moved = lax.rem(row, group) * rows_y + row // group
    weave[...] = jnp.where(moved == lane, 1.0, 0.0).astype(jnp.bfloat16)

    def prepare(h, between=None):
        a, f = order[h]

        def turn(step, carry):
            here = pl.ds(pl.multiple_of(step * block, block), block)
            value = matmul_t(weave[...], raw[a, :, f, here]).astype(jnp.bfloat16)
            rows[h, :, pl.ds(pl.multiple_of(step * group, group), group), :] = value.reshape(rows_y, group, local_k)
            return carry

        if all(order[n][0] != a for n in range(h)):
            span = columns // block // pieces
            for p in range(pieces):
                raw_copies[a][p].wait()
                lax.fori_loop(p * span, (p + 1) * span, turn, 0)
                if between is not None:
                    between(p)
        else:
            lax.fori_loop(0, columns // block, turn, 0)

    my_lanes = pl.ds(pl.multiple_of(j * local_k, local_k), local_k)

    def in_place(h, start=0, count=local_m):
        if shared[h]:
            return held.at[place_of[h], pl.ds(pl.multiple_of(i * local_m, local_m) + start, count), my_lanes]
        return kept.at[place_of[h], pl.ds(pl.multiple_of(member * local_m, local_m) + start, count), my_lanes]

    def send_in(h, row_owner, mode_owner, start=0, count=local_m):
        pltpu.make_async_remote_copy(
            src_ref=rows.at[h, lax.rem(row_owner, members) * ncz + mode_owner, pl.ds(start, count)],
            dst_ref=in_place(h, start, count),
            send_sem=in_send,
            recv_sem=in_recv.at[h],
            device_id=at(row_owner, mode_owner),
            device_id_type=MESH,
        ).start()

    def keep_in(h):
        pltpu.make_async_copy(rows.at[h, my_row], in_place(h), in_recv.at[h]).start()

    def flip(index, step):
        bit = 1
        target = index
        while bit < nkx:
            if step & bit:
                target = target + bit * (1 - 2 * lax.rem(index // bit, 2))
            bit *= 2
        return target

    within = list(range(1, members))
    across = [s for p in range(places - 1, members // 2 - 1, -1) for s in (2 * p + 1, 2 * p)]

    def to_all(steps, send):
        def one(step, carry):
            for s in steps:
                if s:
                    send(flip(i, s), lax.rem(j + step, ncz))
                else:
                    @pl.when(step > 0)
                    def _():
                        send(i, lax.rem(j + step, ncz))
            return carry

        lax.fori_loop(0, ncz, one, 0)

    def hop_away(hops, side_step, use):
        facing = place * 2 + (1 - column if side_step else column)
        if hops == 0:
            use(facing)
        elif hops < places:
            @pl.when(place + hops < places)
            def _():
                use(facing + 2 * hops)

            @pl.when(place >= hops)
            def _():
                use(facing - 2 * hops)

    def each_other(send, target):
        def one(step, carry):
            send(target, lax.rem(j + step, ncz))
            return carry

        lax.fori_loop(1, ncz, one, 0)

    part_m = local_m // pieces

    def begin(p):
        if p == 0:
            pl.semaphore_wait(barrier, near)
            signal_near(ready.at[0])
        if p == pieces - 1:
            for copy in raw_copies[1]:
                copy.start()
        hop_away(1, False, lambda t: send_in(0, t, j, p * part_m, part_m))
        hop_away(0, True, lambda t: send_in(0, t, j, p * part_m, part_m))

    prepare(0, begin)
    send_0 = functools.partial(send_in, 0)
    each_other(send_0, i)
    for distance in range(2, places + 2):
        pl.semaphore_wait(ready.at[distance - 2], near)
        if distance < places + 1:
            signal_near(ready.at[distance - 1])
        if distance <= places:
            hop_away(distance, False, lambda t: send_in(0, t, j))
            hop_away(distance - 1, True, lambda t: send_in(0, t, j))
        hop_away(distance - 1, False, lambda t: each_other(send_0, t))
        hop_away(distance - 2, True, lambda t: each_other(send_0, t))
    keep_in(0)
    table_copy.start()

    def launch(h):
        if h < 2 * fields:
            prepare(h)
            to_all((across if shared[h] else []) + [0] + within, functools.partial(send_in, h))
            keep_in(h)

    for h in range(1, ahead):
        launch(h)

    half_lanes = modes_z // 2
    parts = [slice(n * half_lanes, (n + 1) * half_lanes) for n in range(2)]
    block_z = 256 if points_z % 256 == 0 else points_z

    def own_m(which):
        return pl.ds(pl.multiple_of(which * half_m, half_m), half_m)

    def gather(h, use):
        source = held.at[place_of[h]] if shared[h] else kept.at[place_of[h]]
        wait(source, in_recv.at[h])
        for part in parts:
            table = hartley[...] if shared[h] else hartley[:, own_m(side)]
            mixed[:, part] = matmul(table, source[:, part]).astype(jnp.bfloat16)
        launch(h + ahead)
        lift_table = lifts[order[h][0]]

        def one(step, carry):
            here = pl.ds(pl.multiple_of(step * block_z, block_z), block_z)
            use(here, matmul(mixed[...], lift_table[:, here]))
            return carry

        lax.fori_loop(0, points_z // block_z, one, 0)

    def lower(source):
        for part in parts:
            lowered[:, part] = matmul_t(source[...], lifts[0][part, :]).astype(jnp.bfloat16)

    def out_block(ref, row_owner, mode_owner):
        first_m = pl.multiple_of(lax.rem(row_owner, members) * local_m, local_m)
        return ref.at[pl.ds(first_m, local_m), pl.ds(pl.multiple_of(mode_owner * local_k, local_k), local_k)]

    def send_out(source, target, sem, row_owner, mode_owner):
        pltpu.make_async_remote_copy(
            src_ref=out_block(source, row_owner, mode_owner),
            dst_ref=target,
            send_sem=out_send,
            recv_sem=sem,
            device_id=at(row_owner, mode_owner),
            device_id_type=MESH,
        ).start()

    def finish(f):
        lower(summed if f == 2 else flux)
        if f == 2:
            for part in parts:
                beyond[:, part] = matmul(hartley[own_m(1 - side), :], lowered[:, part]).astype(jnp.bfloat16)
            to_all(across, functools.partial(send_out, beyond, crossed.at[my_row], cross_recv))
        for part in parts:
            result[f, :, part] = matmul(hartley[own_m(side), :], lowered[:, part]).astype(jnp.bfloat16)
        pltpu.make_async_copy(out_block(result.at[f], i, j), landed.at[f, my_row], out_recv.at[f]).start()
        to_all([0] + within, functools.partial(send_out, result.at[f], landed.at[f, my_row], out_recv.at[f]))

    def keep(target):
        def use(here, value):
            target[:, here] = value
        return use

    def multiply(first):
        def use(here, value):
            flux[:, here] = (value * vertical[:, here]).astype(jnp.bfloat16)
            product = value * other[:, here]
            total[:, here] = product if first else total[:, here] + product
        return use

    def double(here, value):
        total[:, here] += 2.0 * value * vertical[:, here]

    def last(here, value):
        flux[:, here] = (value * vertical[:, here]).astype(jnp.bfloat16)
        summed[:, here] = (total[:, here] + value * other[:, here]).astype(jnp.bfloat16)

    table_copy.wait()
    gather(0, keep(vertical))
    gather(1, keep(other))
    gather(2, multiply(True))
    finish(0)
    gather(3, keep(other))
    gather(4, multiply(False))
    finish(1)
    gather(5, keep(other))
    gather(6, double)
    gather(7, last)
    finish(2)
    finish(3)

    def settle(f):
        wait(landed.at[f], out_recv.at[f])
        if f == 2:
            wait(crossed, cross_recv)
        for y in range(rows_y):
            value = landed[f, y].astype(jnp.float32)
            if f == 2:
                value += crossed[y].astype(jnp.float32)
            wide[pl.ds(y, local_m, stride=rows_y), :] = value

        def lay(step, carry):
            here = pl.ds(pl.multiple_of(step * chunk, chunk), chunk)
            stage[step, pl.ds(f, local_k, stride=fields), :] = wide[here, :].T
            if f == 3:
                out[step] = stage[step].astype(jnp.bfloat16)
            return carry

        lax.fori_loop(0, columns // chunk, lay, 0, unroll=f == 3)

    for f in (0, 1, 2, 3):
        settle(f)

    wait(rows.at[pl.ds(0, fields)], in_send)
    wait(rows.at[:, pl.ds(0, rows_y - 1)], in_send)
    wait(landed.at[:, pl.ds(0, rows_y - 1)], out_send)
    wait(crossed, out_send)


def deliver(tiles, out, sem):
    for n in range(tiles.shape[0]):
        pltpu.make_async_copy(tiles.at[n], out.at[:, :, pl.ds(n * 128, 128)], sem).start()
    pltpu.make_async_copy(out, out, sem).wait()


def on_device(nkx, ncz, field_modes, cotangent):
    local_k, fields, columns = field_modes.shape
    local_m = columns // Y
    modes_z, points_x = local_k * ncz, local_m * nkx
    own_rows = Y // nkx
    share_x = points_x // ncz
    bf16 = jnp.bfloat16
    pieces = next(p for p in (3, 2, 1) if columns % (p * 16 * Y) == 0 or p == 1)

    cosines = cosine_table(MZ, modes_z)
    synthesis = (cosines * math.sqrt(2.0 / modes_z)).astype(bf16).T
    projection = (cosines * math.sqrt(2.0 / MZ)).astype(bf16).T
    hartley = hartley_table(points_x).astype(np.float32).astype(bf16)
    tables = jnp.asarray(np.concatenate([hartley, synthesis, projection], axis=0))

    hbm = pl.BlockSpec(memory_space=pltpu.HBM)
    dma = pltpu.SemaphoreType.DMA
    whole_rows = nkx // 2 * ncz == Y and nkx & (nkx - 1) == 0 and local_k % 128 == 0
    if whole_rows:
        members = nkx // 2
        body = kernel_halves
        scratch = [
            pltpu.VMEM((fields, points_x, modes_z), bf16),
            pltpu.VMEM((fields, members * local_m, modes_z), bf16),
            pltpu.VMEM((points_x, modes_z), bf16),
            pltpu.VMEM((points_x, MZ), jnp.float32),
            pltpu.VMEM((points_x, MZ), jnp.float32),
            pltpu.VMEM((points_x, MZ), jnp.float32),
            pltpu.VMEM((points_x, MZ), bf16),
            pltpu.VMEM((points_x, MZ), bf16),
            pltpu.VMEM((points_x, modes_z), bf16),
            pltpu.VMEM((fields, members * local_m, modes_z), bf16),
            pltpu.VMEM((members * local_m, modes_z), bf16),
            pltpu.VMEM((fields, Y, local_m, local_k), bf16),
            pltpu.VMEM((Y, local_m, local_k), bf16),
            dma, dma((2 * fields,)), dma, dma((fields,)), dma,
        ]
    else:
        body = kernel
        scratch = [
            pltpu.VMEM((2 * fields, own_rows, points_x, local_k), bf16),
            pltpu.VMEM((2 * fields, points_x, own_rows * local_k), bf16),
            pltpu.VMEM((2 * fields, ncz, share_x, own_rows * local_k), bf16),
            pltpu.VMEM((fields, own_rows * share_x, MZ), jnp.float32),
            pltpu.VMEM((own_rows * share_x, MZ), jnp.float32),
            pltpu.VMEM((own_rows * share_x, MZ), bf16),
            pltpu.VMEM((fields, ncz, share_x, own_rows * local_k), bf16),
            pltpu.VMEM((fields, points_x, own_rows * local_k), bf16),
            pltpu.VMEM((fields, own_rows, points_x, local_k), bf16),
            pltpu.VMEM((fields, Y, local_m, local_k), bf16),
            dma, dma((2 * fields,)), dma, dma((2 * fields,)),
            dma, dma((fields,)), dma, dma((fields,)),
        ]
    out = pl.pallas_call(
        functools.partial(body, nkx, ncz, pieces),
        out_shape=jax.ShapeDtypeStruct((columns // 128, fields * local_k, 128), bf16),
        in_specs=[hbm] * 3,
        out_specs=pl.BlockSpec(memory_space=pltpu.VMEM),
        scratch_shapes=[
            pltpu.VMEM((2, local_k, fields, columns), bf16),
            pltpu.VMEM(tables.shape, bf16),
            dma((2, pieces)), dma, pltpu.SemaphoreType.REGULAR((nkx // 2 + 1,)),
            pltpu.VMEM((16 * Y, 16 * Y), bf16),
            pltpu.VMEM((columns, local_k), jnp.float32),
            pltpu.VMEM((columns // 128, fields * local_k, 128), jnp.float32),
            pltpu.VMEM((2 * fields, Y, local_m, local_k), bf16),
            *scratch,
        ],
        compiler_params=pltpu.CompilerParams(has_side_effects=True, vmem_limit_bytes=52 * 2**20, collective_id=0),
    )(field_modes, cotangent, tables)
    return pl.pallas_call(
        deliver,
        out_shape=jax.ShapeDtypeStruct(field_modes.shape, bf16),
        in_specs=[pl.BlockSpec(memory_space=pl.ANY)],
        out_specs=hbm,
        scratch_shapes=[dma],
        compiler_params=pltpu.CompilerParams(vmem_limit_bytes=2 * 2**20),
    )(out.reshape(columns // 128, local_k, fields, 128))


def solution(mesh):
    return jax.shard_map(
        functools.partial(on_device, mesh.shape["kx"], mesh.shape["cz"]),
        mesh=mesh,
        in_specs=(P("cz", None, "kx"), P("cz", None, "kx")),
        out_specs=P("cz", None, "kx"),
        check_vma=False,
    )
```
